32 devices in a mesh: dp: 4 (over y, x), seq: 8 (over z, core).
Axes of the slice: x: 2, y: 2, z: 4, core: 2. Of those that a mesh axis runs over, the one named last changes fastest.
Arguments:
- queries: bfloat16 [4, 2048, 16, 128], P('dp', 'seq'), may hold values from -9 to 9
- keys: bfloat16 [4, 2048, 8, 128], P('dp', 'seq'), may hold values from -9 to 9
- values: bfloat16 [4, 2048, 8, 128], P('dp', 'seq'), may hold values from -6 to 6
- doc_lengths: int32 [4, 8], P('dp'), may hold values from 1 to 1536, 2048 in all within a row
Outputs:
- attended: bfloat16 [4, 2048, 16, 128], P('dp', 'seq')
- z_loss: float32 [], replicated
The draws below stay inside these ranges and needn't reach their ends.
Inputs may be any that keep to these rules, and one draw needn't show every extreme that they name: `doc_lengths`: each row's 8 lengths add up to 2048, and its longest document has exactly 1536 tokens.
All inputs are finite; a program needn't handle non-finite values.
Results may differ from the reference program's by a relative error of at most 0.012.
Values may be sent and summed in bfloat16 or wider, within the bound.
A program may use at most 64 MiB of HBM per device.

```python
import math
import jax
import jax.numpy as jnp
import numpy as np
from jax import lax

HQ = 16
KVH = 8
HD = 128
WINDOW = 1024
DOCS = 8
TOK_DEV = 256
BATCH = 4
SEQ_LEN = 2048


def paired_vectors(key):
    query_shape = (BATCH, SEQ_LEN, HQ, HD)
    key_shape = (BATCH, SEQ_LEN, KVH, HD)
    query_draw = 1.5 * jnp.clip(jax.random.normal(jax.random.fold_in(key, 21), query_shape, jnp.float32), -6.0, 6.0)
    key_draw = 1.5 * jnp.clip(jax.random.normal(jax.random.fold_in(key, 22), key_shape, jnp.float32), -6.0, 6.0)
    return (query_draw, key_draw)


def draw_queries(key, part):
    return paired_vectors(key)[0].astype(jnp.bfloat16)


def draw_keys(key, part):
    return paired_vectors(key)[1].astype(jnp.bfloat16)


def steps_of(rng, dims, split, smallest, largest):
    factor_of, own = 1.0, jax.random.fold_in(rng, 6)
    for position, blocks in split:
        heights = jnp.exp(jax.random.uniform(jax.random.fold_in(own, position), (blocks,), jnp.float32, smallest / len(split), largest / len(split)))
        factor_of = factor_of * jnp.repeat(heights, dims[position] // blocks).reshape([-1 if axis == position else 1 for axis in range(len(dims))])
    return factor_of


def split_up(count, total, reach, lean):
    portions = [(1 << 20) // math.isqrt(rank ** lean) + 1 for rank in range(2, count + 1)]
    spare, given = total - reach - (count - 1), [1] * (count - 1)
    while spare > 0:
        candidates = [i for i in range(count - 1) if given[i] < reach]
        whole, left = sum([portions[i] for i in candidates]), spare
        for i in candidates:
            addition = min(reach - given[i], max(1, left * portions[i] // whole), spare)
            given[i] = given[i] + addition
            spare = spare - addition
    return np.array([reach] + given)


def ragged_sizes(rng, count, total, most, lean):
    if count == 2:
        one = jax.random.randint(rng, (), max(1, total - most), min(most, total - 1) + 1)
        return jnp.stack([one, total - one])
    lengths = jnp.asarray(split_up(count, total, most, lean), jnp.int32)
    pairs = (count - 1) // 2
    source_of, taker = lengths[1:1 + 2 * pairs:2], lengths[2:2 + 2 * pairs:2]
    slack = jnp.minimum(source_of - 1, most - taker)
    moved = jax.random.randint(jax.random.fold_in(rng, 1), (pairs,), 0, 1 << 20) % (slack + 1)
    lengths = lengths.at[1:1 + 2 * pairs:2].set(source_of - moved).at[2:2 + 2 * pairs:2].set(taker + moved)
    return lengths[jax.random.permutation(jax.random.fold_in(rng, 2), count)]


def gaussian(stream_key, extent, scale, most, cuts=(), kind=jnp.bfloat16):
    entries = jax.random.normal(stream_key, extent, jnp.float32) * scale
    if len(cuts) > 0:
        entries = steps_of(stream_key, extent, cuts, -0.22, 0.18) * entries
    return jnp.clip(entries, min=-most, max=most).astype(kind)


def setup_inputs(seed: int = 0) -> dict:
    arg_keys = jax.random.split(jax.random.key(seed), 5)
    return {
        "queries": draw_queries(jax.random.fold_in(arg_keys[4], 71), 0),
        "keys": draw_keys(jax.random.fold_in(arg_keys[4], 71), 0),
        "values": gaussian(arg_keys[2], (BATCH, SEQ_LEN, KVH, HD), 1.0, 6.0, ((0, 4), (1, 8))),
        "doc_lengths": jax.vmap(lambda own: ragged_sizes(own, DOCS, SEQ_LEN, 3 * SEQ_LEN // 4, 2))(jax.random.split(arg_keys[3], BATCH)).reshape((BATCH, DOCS)).astype(jnp.int32),
    }


rope_base = 500000.0
score_scale = 1.0 / 12.0
masked = -1.0e30


def rotate(tensor, places):
    half = tensor.shape[-1] // 2
    frequency = rope_base ** (-2.0 * jnp.arange(half, dtype=jnp.float32) / tensor.shape[-1])
    angles = places.astype(jnp.float32)[..., None, None] * frequency
    cos_table = jnp.cos(angles)
    sin_table = jnp.sin(angles)
    widened = tensor.astype(jnp.float32)
    front_half = widened[..., :half]
    back_half = widened[..., half:]
    joined = jnp.concatenate([front_half * cos_table - back_half * sin_table, back_half * cos_table + front_half * sin_table], axis=-1)
    return joined.astype(jnp.bfloat16)


def reference(queries, keys, values, doc_lengths):
    doc_ends = jnp.cumsum(doc_lengths, axis=1)
    doc_starts = doc_ends - doc_lengths
    all_rows = jnp.arange(SEQ_LEN, dtype=jnp.int32)
    doc_of = jnp.sum((doc_ends[:, None, :] <= all_rows[None, :, None]).astype(jnp.int32), axis=2)
    chosen = doc_of[:, :, None] == jnp.arange(DOCS, dtype=jnp.int32)[None, None, :]
    start_of = jnp.sum(jnp.where(chosen, doc_starts[:, None, :], 0), axis=2)
    places = all_rows[None, :] - start_of
    block = 512 if SEQ_LEN % 512 == 0 else TOK_DEV
    group_size = HQ // KVH

    def one_seq(operands):
        seq_queries, seq_keys, seq_values, seq_docs, seq_places = operands
        query_rot = rotate(seq_queries, seq_places)
        key_rot = rotate(seq_keys, seq_places)
        key_padded = jnp.pad(key_rot, ((WINDOW, 0), (0, 0), (0, 0)))
        value_padded = jnp.pad(seq_values, ((WINDOW, 0), (0, 0), (0, 0)))
        docs_padded = jnp.pad(seq_docs, (WINDOW, 0), constant_values=-1)

        def one_block(begin):
            query_block = lax.dynamic_slice_in_dim(query_rot, begin, block, 0).astype(jnp.float32)
            query_block = query_block.reshape(block, KVH, group_size, HD)
            key_block = lax.dynamic_slice_in_dim(key_padded, begin, WINDOW + block, 0).astype(jnp.float32)
            value_block = lax.dynamic_slice_in_dim(value_padded, begin, WINDOW + block, 0).astype(jnp.float32)
            query_docs = lax.dynamic_slice_in_dim(seq_docs, begin, block, 0)
            key_docs = lax.dynamic_slice_in_dim(docs_padded, begin, WINDOW + block, 0)
            query_at = begin + jnp.arange(block, dtype=jnp.int32)
            key_at = begin - WINDOW + jnp.arange(WINDOW + block, dtype=jnp.int32)
            visible = (query_docs[:, None] == key_docs[None, :]) & (key_at[None, :] <= query_at[:, None]) & (query_at[:, None] - key_at[None, :] < WINDOW)
            scores = jnp.einsum("tkgd,ukd->kgtu", query_block, key_block) * score_scale
            scores = jnp.where(visible[None, None], scores, masked)
            peak = jnp.max(scores, axis=-1)
            weights = jnp.where(visible[None, None], jnp.exp(scores - peak[..., None]), 0.0)
            total = jnp.sum(weights, axis=-1)
            rounded = weights.astype(jnp.bfloat16).astype(jnp.float32)
            mixed = jnp.einsum("kgtu,ukd->tkgd", rounded, value_block)
            mixed = mixed / jnp.transpose(total, (2, 0, 1))[..., None]
            return mixed.reshape(block, HQ, HD).astype(jnp.bfloat16), peak + jnp.log(total)

        begins = jnp.arange(SEQ_LEN // block, dtype=jnp.int32) * block
        outputs, normalizers = lax.map(one_block, begins)
        return outputs.reshape(SEQ_LEN, HQ, HD), jnp.sum(normalizers * normalizers)

    attended, squares = lax.map(one_seq, (queries, keys, values, doc_of, places))
    return attended, jnp.sum(squares) / (BATCH * SEQ_LEN * HQ)
```

```python
import functools
import math

import jax
import jax.numpy as jnp
import numpy as np
from jax import lax
from jax.experimental import pallas as pl
from jax.experimental.pallas import tpu as pltpu
from jax.sharding import PartitionSpec as P

WINDOW = 1024
rope_base = 500000.0
score_scale = 1.0 / 12.0
masked = -1e30
MESH = pl.DeviceIdType.MESH
TILE = 64
WIDE = (2, 1)


def tables(rows, n, width):
    half = width // 2
    frequency = rope_base ** (-2.0 * np.arange(half) / width)
    at = np.concatenate([np.arange(rows), rows * np.arange(-(-n // 8) * 8)])
    angles = at[:, None] * frequency
    cos = np.concatenate([np.cos(angles)] * 2, axis=-1)
    sin = np.concatenate([-np.sin(angles), np.sin(angles)], axis=-1)
    return np.stack([cos, sin]).astype(np.float32)


def body(
    n, n_dp, reach, lengths_hbm, q_hbm, k_hbm, v_hbm, tab_hbm, out, z_hbm,
    lengths, z_out, tab, turn, q_raw, raw, stage, spread, q_rot, kv, scores, weights, tops, shares, bias,
    mine, parts_seq, mine2, parts_dp, told, news,
    load_sem, z_send, z_recv, d_send, d_recv, s_send, s_recv, p_send, p_recv, t_send, t_recv,
):
    rows, heads, width = k_hbm.shape
    q_heads = q_hbm.shape[1]
    group = q_heads // heads
    tall = group * rows
    hops = reach // 2
    me = lax.axis_index("seq")
    dp = lax.axis_index("dp")
    core = lax.rem(me, 2)
    chip = me // 2
    other = me + 1 - 2 * core
    above = me + 2
    has_above = above < n
    first = core == 0
    second = core == 1
    blocks = jnp.minimum(me, reach) + 1

    loads = [
        pltpu.make_async_copy(k_hbm, raw.at[0], load_sem.at[0]),
        pltpu.make_async_copy(tab_hbm, tab, load_sem.at[3]),
        pltpu.make_async_copy(v_hbm, raw.at[1], load_sem.at[1]),
        pltpu.make_async_copy(q_hbm, q_raw, load_sem.at[2]),
        pltpu.make_async_copy(lengths_hbm, lengths, load_sem.at[4]),
    ]
    for load in loads:
        load.start()

    barrier = pltpu.get_barrier_semaphore()

    def greet(axis, at):
        pl.semaphore_signal(barrier, inc=1, device_id={axis: at}, device_id_type=MESH)

    def each(low_i, high_i, do):
        def step(i, _):
            do(i)
            return 0

        lax.fori_loop(low_i, high_i, step, 0)

    has_below = me >= 2
    far = me >= 3
    lead = me == 0
    greet("seq", other)
    pl.when(has_above)(lambda: greet("seq", above))
    pl.when(has_below)(lambda: greet("seq", me - 2))

    @pl.when(lead)
    def _():
        each(3, n, lambda j: greet("seq", j))
        each(1, n_dp, lambda j: greet("dp", lax.rem(dp + j, n_dp)))

    greeted = 1 + has_above.astype(jnp.int32) + has_below.astype(jnp.int32) + far.astype(jnp.int32)
    greeted = greeted + lead.astype(jnp.int32) * (n_dp - 1)

    def up(kind, hop, h):
        return pltpu.make_async_remote_copy(
            src_ref=kv.at[kind, 2 * hop, pl.ds(h * WIDE[kind], WIDE[kind])],
            dst_ref=kv.at[kind, 2 * hop + 2, pl.ds(h * WIDE[kind], WIDE[kind])],
            send_sem=z_send.at[kind, hop, h],
            recv_sem=z_recv.at[kind, hop, h],
            device_id={"seq": above},
            device_id_type=MESH,
        )

    def across(kind, hop, h):
        there = 2 * hop + 1 - 2 * core
        slot = hop - core
        return pltpu.make_async_remote_copy(
            src_ref=kv.at[kind, 2 * hop, pl.ds(h * WIDE[kind], WIDE[kind])],
            dst_ref=kv.at[kind, there, pl.ds(h * WIDE[kind], WIDE[kind])],
            send_sem=d_send.at[kind, slot, h],
            recv_sem=d_recv.at[kind, slot, h],
            device_id={"seq": other},
            device_id_type=MESH,
        )

    def send_own(kind, h):
        @pl.when(has_above)
        def _():
            up(kind, 0, h).start()

    def share_own(kind, h):
        @pl.when(first)
        def _():
            across(kind, 0, h).start()

    def take(kind, hop, h):
        up(kind, hop - 1, h).wait_recv()
        if hop < hops:
            @pl.when(has_above)
            def _():
                up(kind, hop, h).start()

            across(kind, hop, h).start()
        else:
            @pl.when(second)
            def _():
                across(kind, hop, h).start()

    def take_across(kind, slot, h):
        pltpu.make_async_remote_copy(
            src_ref=kv.at[kind, 0, pl.ds(h * WIDE[kind], WIDE[kind])],
            dst_ref=kv.at[kind, 2 * slot + 1, pl.ds(h * WIDE[kind], WIDE[kind])],
            send_sem=d_send.at[kind, slot, h],
            recv_sem=d_recv.at[kind, slot, h],
            device_id={"seq": other},
            device_id_type=MESH,
        ).wait_recv()

    loads[0].wait()
    loads[1].wait()
    cos_b = tab[0, pl.ds(rows + me, 1), :]
    sin_b = tab[1, pl.ds(rows + me, 1), :]
    turn[0] = tab[0, 0:rows, :] * cos_b - tab[1, 0:rows, :] * sin_b
    turn[1] = tab[1, 0:rows, :] * cos_b + tab[0, 0:rows, :] * sin_b
    stage[0 : rows * heads, :] = raw[0].astype(jnp.float32).reshape(rows * heads, width)

    def turn_k(h):
        x = stage[pl.ds(h, rows, stride=heads), :]
        kv[0, 0, h] = (x * turn[0] + pltpu.roll(x, width // 2, 1) * turn[1]).astype(jnp.bfloat16)

    wide = WIDE[0]
    k_chunks, v_chunks = heads // WIDE[0], heads // WIDE[1]

    def turn_ks(i):
        for j in range(wide):
            turn_k(i * wide + j)

    turn_ks(0)
    pl.semaphore_wait(barrier, greeted)

    def first_k(i):
        @pl.when(i + 1 < k_chunks)
        def _():
            turn_ks(i + 1)

        send_own(0, i)
        share_own(0, i)

    each(0, k_chunks, first_k)
    loads[4].wait()

    row_at = me * rows + lax.broadcasted_iota(jnp.int32, (rows, rows), 0)
    start = jnp.zeros((rows, rows), jnp.int32)
    end = jnp.int32(0)
    for i in range(lengths.shape[1]):
        end = end + lengths[0, i]
        start = jnp.where(end <= row_at, end, start)
    low = jnp.maximum(start, row_at - (WINDOW - 1)) - me * rows
    query_at = lax.broadcasted_iota(jnp.int32, (rows, rows), 0)
    for d in range(reach + 1):
        key_at = lax.broadcasted_iota(jnp.int32, (rows, rows), 1) - d * rows
        bias[d] = jnp.where((key_at >= low) & (key_at <= query_at), 0.0, masked)

    loads[3].wait()
    stage[...] = q_raw[...].astype(jnp.float32).reshape(rows * q_heads, width)
    scale = score_scale * math.log2(math.e)

    def turn_q(h):
        for g in range(group):
            x = stage[pl.ds(h * group + g, rows, stride=q_heads), :]
            turned = x * turn[0] + pltpu.roll(x, width // 2, 1) * turn[1]
            q_rot[h, g * rows : (g + 1) * rows, :] = (turned * scale).astype(jnp.bfloat16)

    each(0, heads, turn_q)

    loads[2].wait()
    stage[0 : rows * heads, :] = raw[1].astype(jnp.float32).reshape(rows * heads, width)

    def move_v(h):
        kv[1, 0, h] = stage[pl.ds(h, rows, stride=heads), :].astype(jnp.bfloat16)

    each(0, heads, move_v)
    each(0, v_chunks, lambda i: share_own(1, i))

    def score(d, h, fresh=False):
        s = lax.dot_general(
            q_rot[h], kv[0, d, h], (((1,), (1,)), ((), ())), preferred_element_type=jnp.float32
        )
        for g in range(group):
            part = slice(g * rows, (g + 1) * rows)
            t = s[part] + bias[d]
            scores[h, d, part, :] = t
            top = functools.reduce(jnp.maximum, [t[:, i * width : (i + 1) * width] for i in range(rows // width)])
            tops[h, part, :] = top if fresh else jnp.maximum(tops[h, part, :], top)

    def scores_of(d, i):
        each(i * wide, (i + 1) * wide, lambda h: score(d, h))

    each(0, heads, lambda h: score(0, h, fresh=True))

    @pl.when(second)
    def _():
        def step(h):
            take_across(0, 0, h)
            scores_of(1, h)

        each(0, k_chunks, step)

    @pl.when(chip >= 1)
    def _():
        def step(h):
            take(0, 1, h)
            scores_of(2, h)

        each(0, k_chunks, step)

    each(0, v_chunks, lambda i: send_own(1, i))

    @pl.when(chip >= 1)
    def _():
        def step(h):
            take_across(0, core, h)
            scores_of(1 + 2 * core, h)

        each(0, k_chunks, step)

    @pl.when(chip >= 2)
    def _():
        def step(h):
            take(0, 2, h)
            scores_of(4, h)

        each(0, k_chunks, step)

        @pl.when(first)
        def _():
            def step(h):
                take_across(0, 1, h)
                scores_of(3, h)

            each(0, k_chunks, step)

    def finish(h, square, peak, total, part):
        shares[h, part, :] = jnp.broadcast_to(1.0 / total, (total.shape[0], width))
        lse = peak * math.log(2.0) + jnp.log(total)
        return square + jnp.sum(lse * lse, axis=0, keepdims=True)

    def weigh(h, square):
        for i in range(tall // TILE):
            part = slice(i * TILE, (i + 1) * TILE)
            peak = jnp.max(tops[h, part, :], axis=1, keepdims=True)
            total = jnp.zeros((TILE, width), jnp.float32)
            for d in range(reach + 1):
                p = jnp.exp2(scores[h, d, part, :] - peak)
                weights[h, d, part, :] = p.astype(jnp.bfloat16)
                for c in range(rows // width):
                    total = total + p[:, c * width : (c + 1) * width]
            square = finish(h, square, peak, jnp.sum(total, axis=1, keepdims=True), part)
        return square

    def weigh_some(h, square):
        for i in range(tall // TILE):
            part = slice(i * TILE, (i + 1) * TILE)
            peak = jnp.max(tops[h, part, :], axis=1, keepdims=True)

            def step(d, total):
                p = jnp.exp2(scores[h, d, part, :] - peak)
                weights[h, d, part, :] = p.astype(jnp.bfloat16)
                for c in range(rows // width):
                    total = total + p[:, c * width : (c + 1) * width]
                return total

            total = lax.fori_loop(0, blocks, step, jnp.zeros((TILE, width), jnp.float32))
            square = finish(h, square, peak, jnp.sum(total, axis=1, keepdims=True), part)
        return square

    def settle(square):
        mine[...] = jnp.broadcast_to(square, mine.shape)
        parts_seq[me] = jnp.broadcast_to(square, mine.shape)

    @pl.when(chip >= 2)
    def _():
        settle(lax.fori_loop(0, heads, weigh, jnp.zeros((1, 1), jnp.float32)))

    @pl.when(chip < 2)
    def _():
        settle(lax.fori_loop(0, heads, weigh_some, jnp.zeros((1, 1), jnp.float32)))

    def report(j):
        return pltpu.make_async_remote_copy(
            src_ref=mine, dst_ref=parts_seq.at[j], send_sem=s_send.at[0], recv_sem=s_recv.at[j],
            device_id={"seq": 0}, device_id_type=MESH,
        )

    def heard(j):
        return pltpu.make_async_remote_copy(
            src_ref=mine, dst_ref=parts_seq.at[j], send_sem=s_send.at[0], recv_sem=s_recv.at[j],
            device_id={"seq": j}, device_id_type=MESH,
        )

    def tell_dp(j):
        return pltpu.make_async_remote_copy(
            src_ref=mine2, dst_ref=parts_dp.at[dp], send_sem=p_send.at[j], recv_sem=p_recv.at[j],
            device_id={"dp": lax.rem(dp + j, n_dp)}, device_id_type=MESH,
        )

    def heard_dp(j):
        return pltpu.make_async_remote_copy(
            src_ref=mine2, dst_ref=parts_dp.at[lax.rem(dp + n_dp - j, n_dp)], send_sem=p_send.at[j], recv_sem=p_recv.at[j],
            device_id={"dp": lax.rem(dp + j, n_dp)}, device_id_type=MESH,
        )

    def tell(j):
        return pltpu.make_async_remote_copy(
            src_ref=told, dst_ref=news, send_sem=t_send.at[j], recv_sem=t_recv.at[0],
            device_id={"seq": j}, device_id_type=MESH,
        )

    @pl.when(me > 0)
    def _():
        report(me).start()

    @pl.when(chip >= 1)
    def _():
        each(0, v_chunks, lambda i: take(1, 1, i))

    @pl.when(second)
    def _():
        each(0, v_chunks, lambda i: take_across(1, 0, i))

    @pl.when(chip >= 1)
    def _():
        each(0, v_chunks, lambda i: take_across(1, core, i))

    def give(h, o):
        o = o * shares[h]
        for g in range(group):
            spread[pl.ds(h * group + g, rows, stride=q_heads), :] = o[g * rows : (g + 1) * rows]

    def mix(h):
        take(1, 2, h)

        @pl.when(first)
        def _():
            take_across(1, 1, h)

        w = jnp.concatenate([weights[h, d] for d in range(reach + 1)], axis=1)
        v = jnp.concatenate([kv[1, d, h] for d in range(reach + 1)], axis=0)
        give(h, jnp.dot(w, v, preferred_element_type=jnp.float32))

    @pl.when(chip >= 2)
    def _():
        each(0, heads - 1, mix)

    @pl.when(chip < 2)
    def _():
        def mix_some(h):
            def step(d, o):
                return o + jnp.dot(weights[h, d], kv[1, d, h], preferred_element_type=jnp.float32)

            give(h, lax.fori_loop(0, blocks, step, jnp.zeros((tall, width), jnp.float32)))

        each(0, heads, mix_some)

    @pl.when(lead)
    def _():
        each(1, n, lambda j: heard(j).wait_recv())
        column = jnp.sum(parts_seq[...], axis=0)
        mine2[...] = column
        parts_dp[dp] = column
        each(1, n_dp, lambda j: tell_dp(j).start())
        each(1, n_dp, lambda j: heard_dp(j).wait_recv())
        whole = jnp.sum(parts_dp[...], axis=0) / (n_dp * n * rows * q_heads)
        told[...] = whole
        news[...] = whole
        each(1, n, lambda j: tell(j).start())

    @pl.when(me > 0)
    def _():
        tell(me).wait_recv()

    z_out[0, 0] = jnp.sum(news[0:1, 0:1])
    save = pltpu.make_async_copy(z_out, z_hbm, load_sem.at[5])
    save.start()

    def sent_up(kind, hop, a, b):
        each(a, b, lambda i: up(kind, hop, i).wait_send())

    def sent_across(kind, hop, a, b):
        each(a, b, lambda i: across(kind, hop, i).wait_send())

    chunks = (k_chunks, v_chunks)
    for kind in range(2):
        pl.when(has_above)(functools.partial(sent_up, kind, 0, 0, chunks[kind]))
        pl.when(first)(functools.partial(sent_across, kind, 0, 0, chunks[kind]))
        pl.when(chip >= 1)(functools.partial(sent_across, kind, 1, 0, chunks[kind]))
    pl.when(has_above & (chip >= 1))(functools.partial(sent_up, 0, 1, 0, k_chunks))
    pl.when(second & (chip >= 2))(functools.partial(sent_across, 0, 2, 0, k_chunks))

    @pl.when(me > 0)
    def _():
        report(me).wait_send()

    @pl.when(lead)
    def _():
        each(1, n_dp, lambda j: tell_dp(j).wait_send())
        each(1, n, lambda j: tell(j).wait_send())

    @pl.when(chip >= 2)
    def _():
        mix(heads - 1)

    out[...] = spread[...].reshape(rows, q_heads, width).astype(jnp.bfloat16)
    pl.when(has_above & (chip >= 1))(functools.partial(sent_up, 1, 1, 0, v_chunks))
    pl.when(second & (chip >= 2))(functools.partial(sent_across, 1, 2, 0, v_chunks))
    save.wait()


def shards(queries, keys, values, lengths):
    _, rows, q_heads, width = queries.shape
    heads = keys.shape[2]
    group = q_heads // heads
    n = lax.axis_size("seq")
    n_dp = lax.axis_size("dp")
    reach = -(-(WINDOW - 1) // rows)
    assert n % 2 == 0 and reach == 4
    hops = reach // 2
    tab = jnp.asarray(tables(rows, n, width))
    vmem = pl.BlockSpec(memory_space=pltpu.VMEM)
    anywhere = pl.BlockSpec(memory_space=pl.ANY)
    dma = pltpu.SemaphoreType.DMA
    out, z = pl.pallas_call(
        functools.partial(body, n, n_dp, reach),
        out_shape=(
            pltpu.VMEM((rows, q_heads, width), jnp.bfloat16),
            jax.ShapeDtypeStruct((1, 1), jnp.float32),
        ),
        in_specs=[anywhere] * 5,
        out_specs=(vmem, anywhere),
        scratch_shapes=[
            pltpu.SMEM(lengths.shape, jnp.int32),
            pltpu.SMEM((1, 1), jnp.float32),
            pltpu.VMEM(tab.shape, jnp.float32),
            pltpu.VMEM((2, rows, width), jnp.float32),
            pltpu.VMEM((rows, q_heads, width), jnp.bfloat16),
            pltpu.VMEM((2, rows, heads, width), jnp.bfloat16),
            pltpu.VMEM((rows * q_heads, width), jnp.float32),
            pltpu.VMEM((rows * q_heads, width), jnp.float32),
            pltpu.VMEM((heads, group * rows, width), jnp.bfloat16),
            pltpu.VMEM((2, reach + 1, heads, rows, width), jnp.bfloat16),
            pltpu.VMEM((heads, reach + 1, group * rows, rows), jnp.float32),
            pltpu.VMEM((heads, reach + 1, group * rows, rows), jnp.bfloat16),
            pltpu.VMEM((heads, group * rows, width), jnp.float32),
            pltpu.VMEM((heads, group * rows, width), jnp.float32),
            pltpu.VMEM((reach + 1, rows, rows), jnp.float32),
            pltpu.VMEM((8, width), jnp.float32),
            pltpu.VMEM((n, 8, width), jnp.float32),
            pltpu.VMEM((8, width), jnp.float32),
            pltpu.VMEM((n_dp, 8, width), jnp.float32),
            pltpu.VMEM((8, width), jnp.float32),
            pltpu.VMEM((8, width), jnp.float32),
            dma((6,)),
            dma((2, hops, heads)),
            dma((2, hops, heads)),
            dma((2, hops, heads)),
            dma((2, hops, heads)),
            dma((n,)),
            dma((n,)),
            dma((n_dp,)),
            dma((n_dp,)),
            dma((n,)),
            dma((1,)),
        ],
        compiler_params=pltpu.CompilerParams(
            collective_id=0, has_side_effects=True, vmem_limit_bytes=56 * 1024 * 1024
        ),
        name="attend",
    )(lengths, queries[0], keys[0], values[0], tab)
    return out[None], z[0, 0]


def solution(mesh):
    placed = (
        P("dp", "seq", None, None),
        P("dp", "seq", None, None),
        P("dp", "seq", None, None),
        P("dp", None),
    )
    return jax.shard_map(
        shards,
        mesh=mesh,
        in_specs=placed,
        out_specs=(P("dp", "seq", None, None), P()),
        check_vma=False,
    )
```

```python
import functools
import math

import jax
import jax.numpy as jnp
import numpy as np
from jax import lax
from jax.experimental import pallas as pl
from jax.experimental.pallas import tpu as pltpu
from jax.sharding import PartitionSpec as P

WINDOW = 1024
rope_base = 500000.0
score_scale = 1.0 / 12.0
masked = -1e30
MESH = pl.DeviceIdType.MESH
TILE = 64
UP = ((2, 4), (4, 1))
ACROSS = ((4, 4), (4, 1))


def tables(rows, n, width):
    half = width // 2
    frequency = rope_base ** (-2.0 * np.arange(half) / width)
    at = np.concatenate([np.arange(rows), rows * np.arange(-(-n // 8) * 8)])
    angles = at[:, None] * frequency
    cos = np.concatenate([np.cos(angles)] * 2, axis=-1)
    sin = np.concatenate([-np.sin(angles), np.sin(angles)], axis=-1)
    return np.stack([cos, sin]).astype(np.float32)


def body(
    n, n_dp, reach, lengths_hbm, q_hbm, k_hbm, v_hbm, tab_hbm, out, z_out,
    lengths, tab, turn, q_raw, raw, stage, spread, q_rot, kv, scores, weights, tops, shares, bias,
    mine, parts_seq, mine2, parts_dp, told, news,
    load_sem, z_send, z_recv, d_send, d_recv, x_sem, s_sem, p_sem, t_sem,
):
    rows, heads, width = k_hbm.shape
    q_heads = q_hbm.shape[1]
    group = q_heads // heads
    tall = group * rows
    hops = reach // 2
    me = lax.axis_index("seq")
    dp = lax.axis_index("dp")
    core = lax.rem(me, 2)
    chip = me // 2
    other = me + 1 - 2 * core
    above = me + 2
    has_above = above < n
    first = core == 0
    second = core == 1
    blocks = jnp.minimum(me, reach) + 1

    loads = [
        pltpu.make_async_copy(k_hbm, raw.at[0], load_sem.at[0]),
        pltpu.make_async_copy(tab_hbm, tab, load_sem.at[3]),
        pltpu.make_async_copy(v_hbm, raw.at[1], load_sem.at[1]),
        pltpu.make_async_copy(q_hbm, q_raw, load_sem.at[2]),
        pltpu.make_async_copy(lengths_hbm, lengths, load_sem.at[4]),
    ]
    for load in loads[:2]:
        load.start()

    barrier = pltpu.get_barrier_semaphore()

    def greet(axis, at):
        pl.semaphore_signal(barrier, inc=1, device_id={axis: at}, device_id_type=MESH)

    def each(low_i, high_i, do):
        def step(i, _):
            do(i)
            return 0

        lax.fori_loop(low_i, high_i, step, 0)

    has_below = me >= 2
    far = me >= 3
    lead = me == 0
    greet("seq", other)
    pl.when(has_above)(lambda: greet("seq", above))
    pl.when(has_below)(lambda: greet("seq", me - 2))

    @pl.when(lead)
    def _():
        each(3, n, lambda j: greet("seq", j))
        each(1, n_dp, lambda j: greet("dp", lax.rem(dp + j, n_dp)))

    greeted = 1 + has_above.astype(jnp.int32) + has_below.astype(jnp.int32) + far.astype(jnp.int32)
    greeted = greeted + lead.astype(jnp.int32) * (n_dp - 1)

    def places(sizes):
        counts = [[heads // size for size in row] for row in sizes]
        flat = [0] + list(np.cumsum(sum(counts, [])))
        return [[int(flat[kind * hops + j]) for j in range(hops)] for kind in range(2)]

    up_at, across_at = places(UP), places(ACROSS)

    def remote(src, dst, send, recv, axis, at):
        return pltpu.make_async_remote_copy(
            src_ref=src, dst_ref=dst, send_sem=send, recv_sem=recv, device_id={axis: at}, device_id_type=MESH
        )

    def some(kind, d, i, size):
        return kv.at[kind, d, pl.ds(i * size, size)]

    def up(kind, hop, i, size=None):
        size = size or UP[kind][hop]
        return remote(
            some(kind, 2 * hop, i, size), some(kind, 2 * hop + 2, i, size),
            z_send.at[kind * hops + hop], z_recv.at[up_at[kind][hop] + i], "seq", above,
        )

    def across(side, kind, hop, i, size=None):
        slot = hop - side
        size = size or ACROSS[kind][slot]
        return remote(
            some(kind, 2 * hop, i, size), some(kind, 2 * hop + 1 - 2 * side, i, size),
            d_send.at[kind * hops + slot], d_recv.at[across_at[kind][slot] + i], "seq", other,
        )

    def extra_up():
        return remote(
            some(1, 1, heads - 1, 1), some(1, 3, heads - 1, 1), x_sem.at[0], x_sem.at[1], "seq", above
        )

    def extra_across():
        return remote(
            some(1, 3, heads - 1, 1), some(1, 4, heads - 1, 1), x_sem.at[2], x_sem.at[3], "seq", other
        )

    half = heads // 2

    def pieces(i, size):
        return i * (half // size), (i + 1) * (half // size)

    def take_up(kind, hop, i):
        each(*pieces(i, UP[kind][hop]), lambda j: up(kind, hop, j).wait_recv())

    def take_across(kind, slot, i):
        size = ACROSS[kind][slot]

        def one(j):
            remote(
                some(kind, 0, j, size), some(kind, 2 * slot + 1, j, size),
                d_send.at[kind * hops + slot], d_recv.at[across_at[kind][slot] + j], "seq", other,
            ).wait_recv()

        each(*pieces(i, size), one)

    def pass_across(side, kind, hop, i):
        each(*pieces(i, ACROSS[kind][hop - side]), lambda j: across(side, kind, hop, j).start())

    def pass_up(kind, hop, i, short=0):
        a, b = pieces(i, UP[kind][hop])
        each(a, b - short, lambda j: up(kind, hop, j).start())

    loads[0].wait()
    for load in loads[2:]:
        load.start()
    loads[1].wait()
    cos_b = tab[0, pl.ds(rows + me, 1), :]
    sin_b = tab[1, pl.ds(rows + me, 1), :]
    turn[0] = tab[0, 0:rows, :] * cos_b - tab[1, 0:rows, :] * sin_b
    turn[1] = tab[1, 0:rows, :] * cos_b + tab[0, 0:rows, :] * sin_b
    stage[0 : rows * heads, :] = raw[0].astype(jnp.float32).reshape(rows * heads, width)

    def turn_k(h):
        x = stage[pl.ds(h, rows, stride=heads), :]
        kv[0, 0, h] = (x * turn[0] + pltpu.roll(x, width // 2, 1) * turn[1]).astype(jnp.bfloat16)

    wide = UP[0][0]

    def turn_ks(i):
        for j in range(wide):
            turn_k(i * wide + j)

    turn_ks(0)
    pl.semaphore_wait(barrier, greeted)

    def first_k(i):
        @pl.when((i + 1) * wide < heads)
        def _():
            turn_ks(i + 1)

        @pl.when(has_above)
        def _():
            up(0, 0, i).start()

    each(0, heads // wide, first_k)

    @pl.when(first)
    def _():
        for i in range(2):
            pass_across(0, 0, 0, i)

    loads[4].wait()
    row_at = me * rows + lax.broadcasted_iota(jnp.int32, (rows, rows), 0)
    start = jnp.zeros((rows, rows), jnp.int32)
    end = jnp.int32(0)
    for i in range(lengths.shape[1]):
        end = end + lengths[0, i]
        start = jnp.where(end <= row_at, end, start)
    low = jnp.maximum(start, row_at - (WINDOW - 1)) - me * rows
    query_at = lax.broadcasted_iota(jnp.int32, (rows, rows), 0)
    for d in range(reach + 1):
        key_at = lax.broadcasted_iota(jnp.int32, (rows, rows), 1) - d * rows
        bias[d] = jnp.where((key_at >= low) & (key_at <= query_at), 0.0, masked)

    loads[3].wait()
    stage[...] = q_raw[...].astype(jnp.float32).reshape(rows * q_heads, width)
    scale = score_scale * math.log2(math.e)

    def turn_q(h):
        for g in range(group):
            x = stage[pl.ds(h * group + g, rows, stride=q_heads), :]
            turned = x * turn[0] + pltpu.roll(x, width // 2, 1) * turn[1]
            q_rot[h, g * rows : (g + 1) * rows, :] = (turned * scale).astype(jnp.bfloat16)

    each(0, heads, turn_q)

    loads[2].wait()
    stage[0 : rows * heads, :] = raw[1].astype(jnp.float32).reshape(rows * heads, width)

    def move_v(h):
        kv[1, 0, h] = stage[pl.ds(h, rows, stride=heads), :].astype(jnp.bfloat16)

    each(0, heads, move_v)

    @pl.when(first)
    def _():
        for i in range(2):
            pass_across(0, 1, 0, i)

    def score(d, h, fresh=False):
        s = lax.dot_general(
            q_rot[h], kv[0, d, h], (((1,), (1,)), ((), ())), preferred_element_type=jnp.float32
        )
        for g in range(group):
            part = slice(g * rows, (g + 1) * rows)
            t = s[part] + bias[d]
            scores[h, d, part, :] = t
            top = functools.reduce(jnp.maximum, [t[:, i * width : (i + 1) * width] for i in range(rows // width)])
            tops[h, part, :] = top if fresh else jnp.maximum(tops[h, part, :], top)

    def scores_of(d, i):
        each(i * half, (i + 1) * half, lambda h: score(d, h))

    each(0, heads, lambda h: score(0, h, fresh=True))

    @pl.when(second)
    def _():
        def step(i):
            take_across(0, 0, i)
            scores_of(1, i)

        for i in range(2):
            step(i)

    @pl.when(chip >= 1)
    def _():
        for i in range(2):
            take_up(0, 0, i)
            pl.when(has_above)(functools.partial(pass_up, 0, 1, i))
            pl.when(first)(functools.partial(pass_across, 0, 0, 1, i))
            pl.when(second)(functools.partial(pass_across, 1, 0, 1, i))
            scores_of(2, i)

    @pl.when(has_above)
    def _():
        for i in range(2):
            pass_up(1, 0, i)

    @pl.when(chip >= 1)
    def _():
        for i in range(2):
            pl.when(first)(functools.partial(take_across, 0, 0, i))
            pl.when(second)(functools.partial(take_across, 0, 1, i))
            scores_of(1 + 2 * core, i)

    @pl.when(chip >= 2)
    def _():
        for i in range(2):
            take_up(0, 1, i)
            pl.when(second)(functools.partial(pass_across, 1, 0, 2, i))
            scores_of(4, i)

        @pl.when(first)
        def _():
            for i in range(2):
                take_across(0, 1, i)
                scores_of(3, i)

    def finish(h, square, peak, total, part):
        shares[h, part, :] = jnp.broadcast_to(1.0 / total, (total.shape[0], width))
        lse = peak * math.log(2.0) + jnp.log(total)
        return square + jnp.sum(lse * lse, axis=0, keepdims=True)

    def weigh(h, square):
        for i in range(tall // TILE):
            part = slice(i * TILE, (i + 1) * TILE)
            peak = jnp.max(tops[h, part, :], axis=1, keepdims=True)
            total = jnp.zeros((TILE, width), jnp.float32)
            for d in range(reach + 1):
                p = jnp.exp2(scores[h, d, part, :] - peak)
                weights[h, d, part, :] = p.astype(jnp.bfloat16)
                for c in range(rows // width):
                    total = total + p[:, c * width : (c + 1) * width]
            square = finish(h, square, peak, jnp.sum(total, axis=1, keepdims=True), part)
        return square

    def weigh_some(h, square):
        for i in range(tall // TILE):
            part = slice(i * TILE, (i + 1) * TILE)
            peak = jnp.max(tops[h, part, :], axis=1, keepdims=True)

            def step(d, total):
                p = jnp.exp2(scores[h, d, part, :] - peak)
                weights[h, d, part, :] = p.astype(jnp.bfloat16)
                for c in range(rows // width):
                    total = total + p[:, c * width : (c + 1) * width]
                return total

            total = lax.fori_loop(0, blocks, step, jnp.zeros((TILE, width), jnp.float32))
            square = finish(h, square, peak, jnp.sum(total, axis=1, keepdims=True), part)
        return square

    def settle(square):
        mine[...] = jnp.broadcast_to(square, mine.shape)

    @pl.when(chip >= 2)
    def _():
        settle(lax.fori_loop(0, heads, weigh, jnp.zeros((1, 1), jnp.float32)))

    @pl.when(chip < 2)
    def _():
        settle(lax.fori_loop(0, heads, weigh_some, jnp.zeros((1, 1), jnp.float32)))

    def report(j):
        return remote(mine, parts_seq.at[j], s_sem.at[0], s_sem.at[1], "seq", 0)

    def tell_dp(j):
        return remote(mine2, parts_dp.at[dp], p_sem.at[0], p_sem.at[1], "dp", lax.rem(dp + j, n_dp))

    def tell(j):
        return remote(told, news, t_sem.at[0], t_sem.at[1], "seq", j)

    @pl.when(me > 0)
    def _():
        report(me).start()

    @pl.when(chip >= 1)
    def _():
        for i in range(2):
            take_up(1, 0, i)

            @pl.when(first)
            def _(i=i):
                pass_across(0, 1, 1, i)
                if i == 1:
                    for j in range(2):
                        take_across(1, 0, j)

                @pl.when(has_above)
                def _():
                    if i == 1:
                        extra_up().start()
                    pass_up(1, 1, i)

            @pl.when(second)
            def _(i=i):
                pass_across(1, 1, 1, i)
                pl.when(has_above)(functools.partial(pass_up, 1, 1, i, short=i))

    @pl.when(second)
    def _():
        for i in range(2):
            take_across(1, 0, i)

        @pl.when(chip >= 1)
        def _():
            for i in range(2):
                take_across(1, 1, i)

    def give(h, o):
        o = o * shares[h]
        for g in range(group):
            spread[pl.ds(h * group + g, rows, stride=q_heads), :] = o[g * rows : (g + 1) * rows]

    def blend(h, which):
        w = jnp.concatenate([weights[h, d] for d in which], axis=1)
        v = jnp.concatenate([kv[1, d, h] for d in which], axis=0)
        return jnp.dot(w, v, preferred_element_type=jnp.float32)

    def mix(h):
        up(1, 1, h).wait_recv()

        @pl.when(second)
        def _():
            across(1, 1, 2, h).start()

        @pl.when(first)
        def _():
            across(0, 1, 1, h).wait_recv()

        give(h, blend(h, range(reach + 1)))

    last = heads - 1

    @pl.when(chip >= 2)
    def _():
        each(0, half, mix)

        @pl.when(first)
        def _():
            extra_up().wait_recv()
            extra_across().start()

        each(half, last, mix)
        tops[last] = blend(last, range(reach))

    @pl.when(chip < 2)
    def _():
        def mix_some(h):
            def step(d, o):
                return o + jnp.dot(weights[h, d], kv[1, d, h], preferred_element_type=jnp.float32)

            give(h, lax.fori_loop(0, blocks, step, jnp.zeros((tall, width), jnp.float32)))

        each(0, heads, mix_some)

    @pl.when(lead)
    def _():
        parts_seq[0] = mine[...]
        others, peers = parts_seq.at[pl.ds(1, n - 1)], parts_dp.at[pl.ds(1, n_dp - 1)]
        remote(others, others, s_sem.at[0], s_sem.at[1], "seq", other).wait_recv()
        column = jnp.sum(parts_seq[...], axis=0)
        mine2[...] = column
        parts_dp[dp] = column
        each(1, n_dp, lambda j: tell_dp(j).start())
        remote(peers, peers, p_sem.at[0], p_sem.at[1], "seq", other).wait_recv()
        whole = jnp.sum(parts_dp[...], axis=0) / (n_dp * n * rows * q_heads)
        told[...] = whole
        news[...] = whole
        each(1, n, lambda j: tell(j).start())
        remote(peers, peers, p_sem.at[0], p_sem.at[1], "seq", other).wait_send()
        remote(others, others, t_sem.at[0], t_sem.at[1], "seq", other).wait_send()

    @pl.when(me > 0)
    def _():
        tell(me).wait_recv()

    z_out[...] = news[...]

    def sent_up(kind, hop, count=heads):
        up(kind, hop, 0, count).wait_send()

    def sent_across(side, kind, hop, count=heads):
        across(side, kind, hop, 0, count).wait_send()

    for kind in range(2):
        pl.when(has_above)(functools.partial(sent_up, kind, 0))
        pl.when(first)(functools.partial(sent_across, 0, kind, 0))
        pl.when(first & (chip >= 1))(functools.partial(sent_across, 0, kind, 1))
        pl.when(second & (chip >= 1))(functools.partial(sent_across, 1, kind, 1))
    pl.when(has_above & (chip >= 1))(functools.partial(sent_up, 0, 1))
    pl.when(second & (chip >= 2))(functools.partial(sent_across, 1, 0, 2))

    @pl.when(me > 0)
    def _():
        report(me).wait_send()

    @pl.when(chip >= 2)
    def _():
        @pl.when(first)
        def _():
            up(1, 1, last).wait_recv()

        @pl.when(second)
        def _():
            extra_across().wait_recv()

        give(last, tops[last] + blend(last, [reach]))

    out[...] = spread[...].reshape(rows, q_heads, width).astype(jnp.bfloat16)

    @pl.when(chip >= 1)
    def _():
        @pl.when(first & has_above)
        def _():
            sent_up(1, 1)
            extra_up().wait_send()

        pl.when(second & has_above)(functools.partial(sent_up, 1, 1, last))

    @pl.when(chip >= 2)
    def _():
        pl.when(first)(lambda: extra_across().wait_send())
        pl.when(second)(functools.partial(sent_across, 1, 1, 2, last))


def place(held, z_held, out, z_out, z_one, sem):
    copies = [
        pltpu.make_async_copy(held, out, sem.at[0]),
        pltpu.make_async_copy(z_one, z_out, sem.at[1]),
    ]
    copies[0].start()
    z_one[...] = z_held[0:1, 0:1]
    copies[1].start()
    for copy in copies:
        copy.wait()


def shards(queries, keys, values, lengths):
    _, rows, q_heads, width = queries.shape
    heads = keys.shape[2]
    group = q_heads // heads
    n = lax.axis_size("seq")
    n_dp = lax.axis_size("dp")
    reach = -(-(WINDOW - 1) // rows)
    assert n % 2 == 0 and reach == 4 and heads % 8 == 0
    hops = reach // 2
    tab = jnp.asarray(tables(rows, n, width))
    vmem = pl.BlockSpec(memory_space=pltpu.VMEM)
    anywhere = pl.BlockSpec(memory_space=pl.ANY)
    dma = pltpu.SemaphoreType.DMA
    out, z = pl.pallas_call(
        functools.partial(body, n, n_dp, reach),
        out_shape=(
            pltpu.VMEM((rows, q_heads, width), jnp.bfloat16),
            pltpu.VMEM((8, width), jnp.float32),
        ),
        in_specs=[anywhere] * 5,
        out_specs=(vmem, vmem),
        scratch_shapes=[
            pltpu.SMEM(lengths.shape, jnp.int32),
            pltpu.VMEM(tab.shape, jnp.float32),
            pltpu.VMEM((2, rows, width), jnp.float32),
            pltpu.VMEM((rows, q_heads, width), jnp.bfloat16),
            pltpu.VMEM((2, rows, heads, width), jnp.bfloat16),
            pltpu.VMEM((rows * q_heads, width), jnp.float32),
            pltpu.VMEM((rows * q_heads, width), jnp.float32),
            pltpu.VMEM((heads, group * rows, width), jnp.bfloat16),
            pltpu.VMEM((2, reach + 1, heads, rows, width), jnp.bfloat16),
            pltpu.VMEM((heads, reach + 1, group * rows, rows), jnp.float32),
            pltpu.VMEM((heads, reach + 1, group * rows, rows), jnp.bfloat16),
            pltpu.VMEM((heads, group * rows, width), jnp.float32),
            pltpu.VMEM((heads, group * rows, width), jnp.float32),
            pltpu.VMEM((reach + 1, rows, rows), jnp.float32),
            pltpu.VMEM((8, width), jnp.float32),
            pltpu.VMEM((n, 8, width), jnp.float32),
            pltpu.VMEM((8, width), jnp.float32),
            pltpu.VMEM((n_dp, 8, width), jnp.float32),
            pltpu.VMEM((8, width), jnp.float32),
            pltpu.VMEM((8, width), jnp.float32),
            dma((5,)),
            dma((2 * hops,)),
            dma((sum(heads // size for row in UP for size in row),)),
            dma((2 * hops,)),
            dma((sum(heads // size for row in ACROSS for size in row),)),
            dma((4,)),
            dma((2,)),
            dma((2,)),
            dma((2,)),
        ],
        compiler_params=pltpu.CompilerParams(
            collective_id=0, has_side_effects=True, vmem_limit_bytes=56 * 1024 * 1024
        ),
        name="attend",
    )(lengths, queries[0], keys[0], values[0], tab)
    out, z = pl.pallas_call(
        place,
        out_shape=(
            jax.ShapeDtypeStruct((rows, q_heads, width), jnp.bfloat16),
            jax.ShapeDtypeStruct((1, 1), jnp.float32),
        ),
        in_specs=[vmem, vmem],
        out_specs=(anywhere, anywhere),
        scratch_shapes=[pltpu.VMEM((1, 1), jnp.float32), dma((2,))],
        compiler_params=pltpu.CompilerParams(vmem_limit_bytes=4 * 1024 * 1024),
        name="place",
    )(out, z)
    return out[None], z[0, 0]


def solution(mesh):
    placed = (
        P("dp", "seq", None, None),
        P("dp", "seq", None, None),
        P("dp", "seq", None, None),
        P("dp", None),
    )
    return jax.shard_map(
        shards,
        mesh=mesh,
        in_specs=placed,
        out_specs=(P("dp", "seq", None, None), P()),
        check_vma=False,
    )
```

```python
import functools
import math

import jax
import jax.numpy as jnp
import numpy as np
from jax import lax
from jax.experimental import pallas as pl
from jax.experimental.pallas import tpu as pltpu
from jax.sharding import PartitionSpec as P

WINDOW = 1024
rope_base = 500000.0
score_scale = 1.0 / 12.0
masked = -1e30
MESH = pl.DeviceIdType.MESH
TILE = 64
UP = (((2, 2, 2, 2), (4, 4)), ((4, 4), (4, 1, 1, 1)))
ACROSS = (((4, 4), (4, 4)), ((4, 4), (4, 1, 1, 1, 1)))


def tables(rows, n, width):
    half = width // 2
    frequency = rope_base ** (-2.0 * np.arange(half) / width)
    at = np.concatenate([np.arange(rows), rows * np.arange(-(-n // 8) * 8)])
    angles = at[:, None] * frequency
    cos = np.concatenate([np.cos(angles)] * 2, axis=-1)
    sin = np.concatenate([-np.sin(angles), np.sin(angles)], axis=-1)
    return np.stack([cos, sin]).astype(np.float32)


def body(
    n, n_dp, reach, lengths_hbm, q_hbm, k_hbm, v_hbm, tab_hbm, out, z_out,
    lengths, tab, turn, q_raw, lead_raw, raw, stage, spread, q_rot, kv, scores, weights, tops, shares, bias,
    mine, parts_seq, mine2, parts_dp, told, news,
    load_sem, z_send, z_recv, d_send, d_recv, x_recv, s_sem, p_sem, t_sem,
):
    rows, heads, width = k_hbm.shape
    q_heads = q_hbm.shape[1]
    group = q_heads // heads
    tall = group * rows
    hops = reach // 2
    me = lax.axis_index("seq")
    dp = lax.axis_index("dp")
    core = lax.rem(me, 2)
    chip = me // 2
    other = me + 1 - 2 * core
    above = me + 2
    has_above = above < n
    first = core == 0
    second = core == 1
    blocks = jnp.minimum(me, reach) + 1

    wide = heads // len(UP[0][0])
    loads = [
        pltpu.make_async_copy(k_hbm.at[:, 0:wide], lead_raw.at[:, 0:wide], load_sem.at[0]),
        pltpu.make_async_copy(tab_hbm, tab, load_sem.at[3]),
        pltpu.make_async_copy(k_hbm, raw.at[0], load_sem.at[5]),
        pltpu.make_async_copy(v_hbm, raw.at[1], load_sem.at[1]),
        pltpu.make_async_copy(q_hbm, q_raw, load_sem.at[2]),
        pltpu.make_async_copy(lengths_hbm, lengths, load_sem.at[4]),
    ]
    for load in loads[:3]:
        load.start()

    barrier = pltpu.get_barrier_semaphore()

    def greet(axis, at):
        pl.semaphore_signal(barrier, inc=1, device_id={axis: at}, device_id_type=MESH)

    def each(low_i, high_i, do):
        def step(i, _):
            do(i)
            return 0

        lax.fori_loop(low_i, high_i, step, 0)

    has_below = me >= 2
    far = me >= 3
    lead = me == 0
    greet("seq", other)
    pl.when(has_above)(lambda: greet("seq", above))
    pl.when(has_below)(lambda: greet("seq", me - 2))

    @pl.when(lead)
    def _():
        each(3, n, lambda j: greet("seq", j))
        each(1, n_dp, lambda j: greet("dp", lax.rem(dp + j, n_dp)))

    greeted = 1 + has_above.astype(jnp.int32) + has_below.astype(jnp.int32) + far.astype(jnp.int32)
    greeted = greeted + lead.astype(jnp.int32) * (n_dp - 1)

    def lay(table):
        count = 0
        laid = []
        for row in table:
            for eighths in row:
                at, cuts = 0, []
                for size in eighths:
                    cuts.append((count, at * heads // 8, size * heads // 8))
                    count, at = count + 1, at + size
                laid.append(cuts)
        return laid

    up_cuts, across_cuts = lay(UP), lay(ACROSS)

    def remote(src, dst, send, recv, axis, at):
        return pltpu.make_async_remote_copy(
            src_ref=src, dst_ref=dst, send_sem=send, recv_sem=recv, device_id={axis: at}, device_id_type=MESH
        )

    def some(kind, d, i, size):
        return kv.at[kind, d, pl.ds(i, size)]

    def up(kind, hop, cut):
        at, start, size = cut
        late = kind * hop
        return remote(
            some(kind, 2 * hop, start, size), some(kind, 2 * hop + 2, start, size),
            z_send.at[late], z_recv.at[at], "seq", above,
        )

    def across(side, kind, hop, cut):
        at, start, size = cut
        late = int(kind == 1 and hop == 2)
        return remote(
            some(kind, 2 * hop, start, size), some(kind, 2 * hop + 1 - 2 * side, start, size),
            d_send.at[late], d_recv.at[at], "seq", other,
        )

    last = heads - 1

    def lend_up():
        return remote(some(1, 1, last, 1), some(1, 3, last, 1), z_send.at[1], x_recv.at[0], "seq", above)

    def lend_across():
        return remote(some(1, 3, last, 1), some(1, 4, last, 1), d_send.at[1], x_recv.at[1], "seq", other)

    def cross_up(j):
        h = last - 1 + j
        return remote(some(1, 3, h, 1), some(1, 4, h, 1), z_send.at[1], x_recv.at[2 + j], "seq", me + 1)

    half = heads // 2

    def cuts_of(cuts, i):
        return [cut for cut in cuts if i * half <= cut[1] < (i + 1) * half]

    def take_up(kind, hop, i):
        for cut in cuts_of(up_cuts[kind * hops + hop], i):
            up(kind, hop, cut).wait_recv()

    def take_cut(kind, slot, cut):
        at, start, size = cut
        remote(
            some(kind, 0, start, size), some(kind, 2 * slot + 1, start, size),
            d_send.at[0], d_recv.at[at], "seq", other,
        ).wait_recv()

    def take_across(kind, slot, i):
        for cut in cuts_of(across_cuts[kind * hops + slot], i):
            take_cut(kind, slot, cut)

    def pass_across(side, kind, hop, i):
        for cut in cuts_of(across_cuts[kind * hops + hop - side], i):
            across(side, kind, hop, cut).start()

    def pass_up(kind, hop, i, short=0):
        cuts = cuts_of(up_cuts[kind * hops + hop], i)
        for cut in cuts[: len(cuts) - short]:
            up(kind, hop, cut).start()

    loads[0].wait()
    loads[1].wait()
    cos_b = tab[0, pl.ds(rows + me, 1), :]
    sin_b = tab[1, pl.ds(rows + me, 1), :]
    turn[0] = tab[0, 0:rows, :] * cos_b - tab[1, 0:rows, :] * sin_b
    turn[1] = tab[1, 0:rows, :] * cos_b + tab[0, 0:rows, :] * sin_b
    stage[0 : rows * heads, :] = lead_raw[...].astype(jnp.float32).reshape(rows * heads, width)

    def turn_k(h):
        x = stage[pl.ds(h, rows, stride=heads), :]
        kv[0, 0, h] = (x * turn[0] + pltpu.roll(x, width // 2, 1) * turn[1]).astype(jnp.bfloat16)

    def turn_ks(i):
        for j in range(wide):
            turn_k(i * wide + j)

    turn_ks(0)
    pl.semaphore_wait(barrier, greeted)

    def send_k(i):
        pl.when(has_above)(lambda: up(0, 0, up_cuts[0][i]).start())

    send_k(0)
    loads[2].wait()
    for load in loads[3:]:
        load.start()
    stage[0 : rows * heads, :] = raw[0].astype(jnp.float32).reshape(rows * heads, width)
    turn_ks(1)
    for i in range(1, len(up_cuts[0])):
        if i + 1 < len(up_cuts[0]):
            turn_ks(i + 1)
        send_k(i)

    @pl.when(first)
    def _():
        for i in range(2):
            pass_across(0, 0, 0, i)

    loads[5].wait()
    row_at = me * rows + lax.broadcasted_iota(jnp.int32, (rows, rows), 0)
    start = jnp.zeros((rows, rows), jnp.int32)
    end = jnp.int32(0)
    for i in range(lengths.shape[1]):
        end = end + lengths[0, i]
        start = jnp.where(end <= row_at, end, start)
    low = jnp.maximum(start, row_at - (WINDOW - 1)) - me * rows
    query_at = lax.broadcasted_iota(jnp.int32, (rows, rows), 0)
    for d in range(reach + 1):
        key_at = lax.broadcasted_iota(jnp.int32, (rows, rows), 1) - d * rows
        bias[d] = jnp.where((key_at >= low) & (key_at <= query_at), 0.0, masked)

    loads[4].wait()
    stage[...] = q_raw[...].astype(jnp.float32).reshape(rows * q_heads, width)
    scale = score_scale * math.log2(math.e)

    def turn_q(h):
        for g in range(group):
            x = stage[pl.ds(h * group + g, rows, stride=q_heads), :]
            turned = x * turn[0] + pltpu.roll(x, width // 2, 1) * turn[1]
            q_rot[h, g * rows : (g + 1) * rows, :] = (turned * scale).astype(jnp.bfloat16)

    each(0, heads, turn_q)

    loads[3].wait()
    stage[0 : rows * heads, :] = raw[1].astype(jnp.float32).reshape(rows * heads, width)

    def move_v(h):
        kv[1, 0, h] = stage[pl.ds(h, rows, stride=heads), :].astype(jnp.bfloat16)

    each(0, heads, move_v)

    @pl.when(first)
    def _():
        for i in range(2):
            pass_across(0, 1, 0, i)

    def score(d, h, fresh=False):
        s = lax.dot_general(
            q_rot[h], kv[0, d, h], (((1,), (1,)), ((), ())), preferred_element_type=jnp.float32
        )
        for g in range(group):
            part = slice(g * rows, (g + 1) * rows)
            t = s[part] + bias[d]
            scores[h, d, part, :] = t
            top = functools.reduce(jnp.maximum, [t[:, i * width : (i + 1) * width] for i in range(rows // width)])
            tops[h, part, :] = top if fresh else jnp.maximum(tops[h, part, :], top)

    def scores_of(d, i):
        each(i * half, (i + 1) * half, lambda h: score(d, h))

    each(0, heads, lambda h: score(0, h, fresh=True))

    @pl.when(second)
    def _():
        def step(i):
            take_across(0, 0, i)
            scores_of(1, i)

        for i in range(2):
            step(i)

    @pl.when(chip >= 1)
    def _():
        for i in range(2):
            take_up(0, 0, i)
            pl.when(has_above)(functools.partial(pass_up, 0, 1, i))
            pl.when(first)(functools.partial(pass_across, 0, 0, 1, i))
            pl.when(second)(functools.partial(pass_across, 1, 0, 1, i))
            scores_of(2, i)

    @pl.when(has_above)
    def _():
        for i in range(2):
            pass_up(1, 0, i)

    @pl.when(chip >= 1)
    def _():
        for i in range(2):
            pl.when(first)(functools.partial(take_across, 0, 0, i))
            pl.when(second)(functools.partial(take_across, 0, 1, i))
            scores_of(1 + 2 * core, i)

    @pl.when(chip >= 2)
    def _():
        for i in range(2):
            take_up(0, 1, i)
            pl.when(second)(functools.partial(pass_across, 1, 0, 2, i))
            scores_of(4, i)

        @pl.when(first)
        def _():
            for i in range(2):
                take_across(0, 1, i)
                scores_of(3, i)

    def finish(h, square, peak, total, part):
        shares[h, part, :] = jnp.broadcast_to(1.0 / total, (total.shape[0], width))
        lse = peak * math.log(2.0) + jnp.log(total)
        return square + jnp.sum(lse * lse, axis=0, keepdims=True)

    def weigh(h, square):
        for i in range(tall // TILE):
            part = slice(i * TILE, (i + 1) * TILE)
            peak = jnp.max(tops[h, part, :], axis=1, keepdims=True)
            total = jnp.zeros((TILE, width), jnp.float32)
            for d in range(reach + 1):
                p = jnp.exp2(scores[h, d, part, :] - peak)
                weights[h, d, part, :] = p.astype(jnp.bfloat16)
                for c in range(rows // width):
                    total = total + p[:, c * width : (c + 1) * width]
            square = finish(h, square, peak, jnp.sum(total, axis=1, keepdims=True), part)
        return square

    def weigh_some(h, square):
        for i in range(tall // TILE):
            part = slice(i * TILE, (i + 1) * TILE)
            peak = jnp.max(tops[h, part, :], axis=1, keepdims=True)

            def step(d, total):
                p = jnp.exp2(scores[h, d, part, :] - peak)
                weights[h, d, part, :] = p.astype(jnp.bfloat16)
                for c in range(rows // width):
                    total = total + p[:, c * width : (c + 1) * width]
                return total

            total = lax.fori_loop(0, blocks, step, jnp.zeros((TILE, width), jnp.float32))
            square = finish(h, square, peak, jnp.sum(total, axis=1, keepdims=True), part)
        return square

    def settle(square):
        mine[...] = jnp.broadcast_to(square, mine.shape)

    @pl.when(chip >= 2)
    def _():
        settle(lax.fori_loop(0, heads, weigh, jnp.zeros((1, 1), jnp.float32)))

    @pl.when(chip < 2)
    def _():
        settle(lax.fori_loop(0, heads, weigh_some, jnp.zeros((1, 1), jnp.float32)))

    def report(j):
        return remote(mine, parts_seq.at[j], s_sem.at[0], s_sem.at[1], "seq", 0)

    def tell_dp(j):
        return remote(mine2, parts_dp.at[dp], p_sem.at[0], p_sem.at[1], "dp", lax.rem(dp + j, n_dp))

    def tell(j):
        return remote(told, news, t_sem.at[0], t_sem.at[1], "seq", j)

    @pl.when(me > 0)
    def _():
        report(me).start()

    @pl.when(chip >= 1)
    def _():
        for i in range(2):
            take_up(1, 0, i)

            @pl.when(first)
            def _(i=i):
                pass_across(0, 1, 1, i)
                if i == 1:
                    for j in range(2):
                        take_across(1, 0, j)
                    pl.when(has_above)(lambda: lend_up().start())
                pl.when(has_above)(functools.partial(pass_up, 1, 1, i, short=i))

            @pl.when(second)
            def _(i=i):
                pl.when(has_above)(functools.partial(pass_up, 1, 1, i))
                pass_across(1, 1, 1, i)

    @pl.when(second)
    def _():
        for i in range(2):
            take_across(1, 0, i)

        @pl.when(chip >= 1)
        def _():
            for i in range(2):
                take_across(1, 1, i)

            @pl.when(has_above)
            def _():
                for j in range(2):
                    cross_up(j).start()

    def give(h, o):
        o = o * shares[h]
        for g in range(group):
            spread[pl.ds(h * group + g, rows, stride=q_heads), :] = o[g * rows : (g + 1) * rows]

    def blend(h, which):
        w = jnp.concatenate([weights[h, d] for d in which], axis=1)
        v = jnp.concatenate([kv[1, d, h] for d in which], axis=0)
        return jnp.dot(w, v, preferred_element_type=jnp.float32)

    def mix(h):
        give(h, tops[h] + blend(h, (reach - 1, reach)))

    def mix_early(h):
        tops[h] = blend(h, range(reach - 1))

    @pl.when(chip >= 2)
    def _():
        each(0, heads, mix_early)
        ups, acrosses = up_cuts[-1], across_cuts[-1]

        def mixed(cut):
            each(cut[1], cut[1] + cut[2], mix)

        @pl.when(first)
        def _():
            for j in range(2):
                up(1, 1, ups[j]).wait_recv()
                take_cut(1, 1, acrosses[j])
                mixed(ups[j])
                if j == 0:
                    lend_up().wait_recv()
                    lend_across().start()

            cross_up(0).wait_recv()
            take_cut(1, 1, acrosses[3])
            mixed(ups[3])
            up(1, 1, ups[2]).wait_recv()
            take_cut(1, 1, acrosses[2])
            mixed(ups[2])

        @pl.when(second)
        def _():
            for j in range(4):
                up(1, 1, ups[j]).wait_recv()
                across(1, 1, 2, acrosses[j]).start()
                mixed(ups[j])

    @pl.when(chip < 2)
    def _():
        def mix_some(h):
            def step(d, o):
                return o + jnp.dot(weights[h, d], kv[1, d, h], preferred_element_type=jnp.float32)

            give(h, lax.fori_loop(0, blocks, step, jnp.zeros((tall, width), jnp.float32)))

        each(0, heads, mix_some)

    @pl.when(lead)
    def _():
        parts_seq[0] = mine[...]
        others, peers = parts_seq.at[pl.ds(1, n - 1)], parts_dp.at[pl.ds(1, n_dp - 1)]
        remote(others, others, s_sem.at[0], s_sem.at[1], "seq", other).wait_recv()
        column = jnp.sum(parts_seq[...], axis=0)
        mine2[...] = column
        parts_dp[dp] = column
        each(1, n_dp, lambda j: tell_dp(j).start())
        remote(peers, peers, p_sem.at[0], p_sem.at[1], "seq", other).wait_recv()
        whole = jnp.sum(parts_dp[...], axis=0) / (n_dp * n * rows * q_heads)
        told[...] = whole
        news[...] = whole
        each(1, n, lambda j: tell(j).start())
        remote(peers, peers, p_sem.at[0], p_sem.at[1], "seq", other).wait_send()
        remote(others, others, t_sem.at[0], t_sem.at[1], "seq", other).wait_send()

    @pl.when(me > 0)
    def _():
        tell(me).wait_recv()

    z_out[...] = news[...]

    def sent(view, sem):
        remote(view, view, sem, sem, "seq", other).wait_send()

    pl.when(has_above & (chip == 0))(lambda: sent(kv.at[0, 0:2], z_send.at[0]))
    pl.when(has_above & (chip >= 1))(lambda: sent(kv.at[0, 0:3], z_send.at[0]))
    pl.when(first & (chip == 0))(lambda: sent(kv.at[0, 0:2], d_send.at[0]))
    pl.when(first & (chip >= 1))(lambda: sent(kv.at[0, 0:4], d_send.at[0]))
    pl.when(second & (chip == 1))(lambda: sent(kv.at[0, 0:2], d_send.at[0]))
    pl.when(second & (chip >= 2))(lambda: sent(kv.at[0, 0:3], d_send.at[0]))

    @pl.when(me > 0)
    def _():
        report(me).wait_send()

    @pl.when(chip >= 2)
    def _():
        @pl.when(first)
        def _():
            cross_up(1).wait_recv()
            mix(last)

        @pl.when(second)
        def _():
            lend_across().wait_recv()
            mix(last)

    out[...] = spread[...].reshape(rows, q_heads, width).astype(jnp.bfloat16)

    pl.when(first & has_above & (chip >= 1))(lambda: sent(kv.at[1, 0, 0:last], z_send.at[1]))
    pl.when(second & has_above & (chip >= 1))(lambda: sent(kv.at[1, 0:3, 0 : (heads + 1) // 3], z_send.at[1]))
    pl.when(first & (chip >= 2))(lambda: sent(kv.at[1, 0, 0:1], d_send.at[1]))
    pl.when(second & (chip >= 2))(lambda: sent(kv.at[1, 0, 0:last], d_send.at[1]))


def place(held, z_held, out, z_out, z_one, sem):
    copies = [
        pltpu.make_async_copy(held, out, sem.at[0]),
        pltpu.make_async_copy(z_one, z_out, sem.at[1]),
    ]
    copies[0].start()
    z_one[...] = z_held[0:1, 0:1]
    copies[1].start()
    for copy in copies:
        copy.wait()


def shards(queries, keys, values, lengths):
    _, rows, q_heads, width = queries.shape
    heads = keys.shape[2]
    group = q_heads // heads
    n = lax.axis_size("seq")
    n_dp = lax.axis_size("dp")
    reach = -(-(WINDOW - 1) // rows)
    assert n % 2 == 0 and reach == 4 and heads == 8
    hops = reach // 2
    tab = jnp.asarray(tables(rows, n, width))
    vmem = pl.BlockSpec(memory_space=pltpu.VMEM)
    anywhere = pl.BlockSpec(memory_space=pl.ANY)
    dma = pltpu.SemaphoreType.DMA
    out, z = pl.pallas_call(
        functools.partial(body, n, n_dp, reach),
        out_shape=(
            pltpu.VMEM((rows, q_heads, width), jnp.bfloat16),
            pltpu.VMEM((8, width), jnp.float32),
        ),
        in_specs=[anywhere] * 5,
        out_specs=(vmem, vmem),
        scratch_shapes=[
            pltpu.SMEM(lengths.shape, jnp.int32),
            pltpu.VMEM(tab.shape, jnp.float32),
            pltpu.VMEM((2, rows, width), jnp.float32),
            pltpu.VMEM((rows, q_heads, width), jnp.bfloat16),
            pltpu.VMEM((rows, heads, width), jnp.bfloat16),
            pltpu.VMEM((2, rows, heads, width), jnp.bfloat16),
            pltpu.VMEM((rows * q_heads, width), jnp.float32),
            pltpu.VMEM((rows * q_heads, width), jnp.float32),
            pltpu.VMEM((heads, group * rows, width), jnp.bfloat16),
            pltpu.VMEM((2, reach + 1, heads, rows, width), jnp.bfloat16),
            pltpu.VMEM((heads, reach + 1, group * rows, rows), jnp.float32),
            pltpu.VMEM((heads, reach + 1, group * rows, rows), jnp.bfloat16),
            pltpu.VMEM((heads, group * rows, width), jnp.float32),
            pltpu.VMEM((heads, group * rows, width), jnp.float32),
            pltpu.VMEM((reach + 1, rows, rows), jnp.float32),
            pltpu.VMEM((8, width), jnp.float32),
            pltpu.VMEM((n, 8, width), jnp.float32),
            pltpu.VMEM((8, width), jnp.float32),
            pltpu.VMEM((n_dp, 8, width), jnp.float32),
            pltpu.VMEM((8, width), jnp.float32),
            pltpu.VMEM((8, width), jnp.float32),
            dma((6,)),
            dma((2,)),
            dma((sum(len(cuts) for row in UP for cuts in row),)),
            dma((2,)),
            dma((sum(len(cuts) for row in ACROSS for cuts in row),)),
            dma((4,)),
            dma((2,)),
            dma((2,)),
            dma((2,)),
        ],
        compiler_params=pltpu.CompilerParams(
            collective_id=0, has_side_effects=True, vmem_limit_bytes=56 * 1024 * 1024
        ),
        name="attend",
    )(lengths, queries[0], keys[0], values[0], tab)
    out, z = pl.pallas_call(
        place,
        out_shape=(
            jax.ShapeDtypeStruct((rows, q_heads, width), jnp.bfloat16),
            jax.ShapeDtypeStruct((1, 1), jnp.float32),
        ),
        in_specs=[vmem, vmem],
        out_specs=(anywhere, anywhere),
        scratch_shapes=[pltpu.VMEM((1, 1), jnp.float32), dma((2,))],
        compiler_params=pltpu.CompilerParams(vmem_limit_bytes=4 * 1024 * 1024),
        name="place",
    )(out, z)
    return out[None], z[0, 0]


def solution(mesh):
    placed = (
        P("dp", "seq", None, None),
        P("dp", "seq", None, None),
        P("dp", "seq", None, None),
        P("dp", None),
    )
    return jax.shard_map(
        shards,
        mesh=mesh,
        in_specs=placed,
        out_specs=(P("dp", "seq", None, None), P()),
        check_vma=False,
    )
```

```python
import functools
import math

import jax
import jax.numpy as jnp
import numpy as np
from jax import lax
from jax.experimental import pallas as pl
from jax.experimental.pallas import tpu as pltpu
from jax.sharding import PartitionSpec as P

WINDOW = 1024
rope_base = 500000.0
score_scale = 1.0 / 12.0
masked = -1e30
MESH = pl.DeviceIdType.MESH
TILE = 64
PARTS = 4
UP = (((2, 2, 2, 2), (4, 4)), ((4, 4), (4, 1, 1, 1)))
ACROSS = (((4, 4), (4, 4)), ((4, 4), (4, 1, 1, 1, 1)))


def tables(rows, n, width):
    half = width // 2
    frequency = rope_base ** (-2.0 * np.arange(half) / width)
    at = np.concatenate([np.arange(rows), rows * np.arange(-(-n // 8) * 8)])
    angles = at[:, None] * frequency
    cos = np.concatenate([np.cos(angles)] * 2, axis=-1)
    sin = np.concatenate([-np.sin(angles), np.sin(angles)], axis=-1)
    return np.stack([cos, sin]).astype(np.float32)


def body(
    n, n_dp, reach, lengths_hbm, q_hbm, k_hbm, v_hbm, tab_hbm, spread, z_out,
    lengths, tab, turn, q_raw, lead_raw, raw, stage, q_rot, kv, scores, weights, tops, shares, bias,
    mine, parts_seq, mine2, parts_dp, told, news,
    load_sem, z_send, z_recv, d_send, d_recv, x_recv, s_sem, p_sem,
):
    rows, heads, width = k_hbm.shape
    q_heads = q_hbm.shape[1]
    group = q_heads // heads
    tall = group * rows
    hops = reach // 2
    me = lax.axis_index("seq")
    dp = lax.axis_index("dp")
    core = lax.rem(me, 2)
    chip = me // 2
    other = me + 1 - 2 * core
    above = me + 2
    has_above = above < n
    first = core == 0
    second = core == 1
    blocks = jnp.minimum(me, reach) + 1

    wide = heads // len(UP[0][0])
    loads = [
        pltpu.make_async_copy(k_hbm.at[:, 0:wide], lead_raw.at[:, 0:wide], load_sem.at[0]),
        pltpu.make_async_copy(tab_hbm, tab, load_sem.at[0]),
        pltpu.make_async_copy(k_hbm, raw.at[0], load_sem.at[1]),
        pltpu.make_async_copy(v_hbm, raw.at[1], load_sem.at[2]),
        pltpu.make_async_copy(q_hbm, q_raw, load_sem.at[2]),
        pltpu.make_async_copy(lengths_hbm, lengths, load_sem.at[3]),
    ]
    for load in loads[:3]:
        load.start()

    barrier = pltpu.get_barrier_semaphore()

    def greet(axis, at):
        pl.semaphore_signal(barrier, inc=1, device_id={axis: at}, device_id_type=MESH)

    def each(low_i, high_i, do):
        def step(i, _):
            do(i)
            return 0

        lax.fori_loop(low_i, high_i, step, 0)

    has_below = me >= 2
    far = me >= 3
    lead = me == 0
    greet("seq", other)
    pl.when(has_above)(lambda: greet("seq", above))
    pl.when(has_below)(lambda: greet("seq", me - 2))

    @pl.when(lead)
    def _():
        each(3, n, lambda j: greet("seq", j))
        each(1, n_dp, lambda j: greet("dp", lax.rem(dp + j, n_dp)))

    greeted = 1 + has_above.astype(jnp.int32) + has_below.astype(jnp.int32) + far.astype(jnp.int32)
    greeted = greeted + lead.astype(jnp.int32) * (n_dp - 1)

    def lay(table):
        count = 0
        laid = []
        for row in table:
            for eighths in row:
                at, cuts = 0, []
                for size in eighths:
                    cuts.append((count, at * heads // 8, size * heads // 8))
                    count, at = count + 1, at + size
                laid.append(cuts)
        return laid

    up_cuts, across_cuts = lay(UP), lay(ACROSS)

    def remote(src, dst, send, recv, axis, at):
        return pltpu.make_async_remote_copy(
            src_ref=src, dst_ref=dst, send_sem=send, recv_sem=recv, device_id={axis: at}, device_id_type=MESH
        )

    def some(kind, d, i, size):
        return kv.at[kind, d, pl.ds(i, size)]

    def up(kind, hop, cut):
        at, start, size = cut
        late = kind * hop
        return remote(
            some(kind, 2 * hop, start, size), some(kind, 2 * hop + 2, start, size),
            z_send.at[late], z_recv.at[at], "seq", above,
        )

    def across(side, kind, hop, cut):
        at, start, size = cut
        late = int(kind == 1 and hop == 2)
        return remote(
            some(kind, 2 * hop, start, size), some(kind, 2 * hop + 1 - 2 * side, start, size),
            d_send.at[late], d_recv.at[at], "seq", other,
        )

    last = heads - 1

    def lend_up():
        return remote(some(1, 1, last, 1), some(1, 3, last, 1), z_send.at[1], x_recv.at[0], "seq", above)

    def lend_across():
        return remote(some(1, 3, last, 1), some(1, 4, last, 1), d_send.at[1], x_recv.at[0], "seq", other)

    def cross_up(j):
        h = last - 1 + j
        landed = x_recv.at[1] if j else z_recv.at[up_cuts[-1][-1][0]]
        return remote(some(1, 3, h, 1), some(1, 4, h, 1), z_send.at[1], landed, "seq", me + 1)

    half = heads // 2

    def cuts_of(cuts, i):
        return [cut for cut in cuts if i * half <= cut[1] < (i + 1) * half]

    def take_up(kind, hop, i):
        for cut in cuts_of(up_cuts[kind * hops + hop], i):
            up(kind, hop, cut).wait_recv()

    def take_cut(kind, slot, cut):
        at, start, size = cut
        remote(
            some(kind, 0, start, size), some(kind, 2 * slot + 1, start, size),
            d_send.at[0], d_recv.at[at], "seq", other,
        ).wait_recv()

    def take_across(kind, slot, i):
        for cut in cuts_of(across_cuts[kind * hops + slot], i):
            take_cut(kind, slot, cut)

    def pass_across(side, kind, hop, i):
        for cut in cuts_of(across_cuts[kind * hops + hop - side], i):
            across(side, kind, hop, cut).start()

    def pass_up(kind, hop, i, short=0):
        cuts = cuts_of(up_cuts[kind * hops + hop], i)
        for cut in cuts[: len(cuts) - short]:
            up(kind, hop, cut).start()

    def loaded(sem, *sizes):
        view = stage.at[0 : sum(sizes) // (4 * width)]
        pltpu.make_async_copy(view, view, sem).wait()

    loaded(load_sem.at[0], 2 * rows * wide * width, 4 * 2 * tab.shape[1] * width)
    cos_b = tab[0, pl.ds(rows + me, 1), :]
    sin_b = tab[1, pl.ds(rows + me, 1), :]
    turn[0] = tab[0, 0:rows, :] * cos_b - tab[1, 0:rows, :] * sin_b
    turn[1] = tab[1, 0:rows, :] * cos_b + tab[0, 0:rows, :] * sin_b
    stage[0 : rows * heads, :] = lead_raw[...].astype(jnp.float32).reshape(rows * heads, width)

    def turn_k(h):
        x = stage[pl.ds(h, rows, stride=heads), :]
        kv[0, 0, h] = (x * turn[0] + pltpu.roll(x, width // 2, 1) * turn[1]).astype(jnp.bfloat16)

    def turn_ks(i):
        for j in range(wide):
            turn_k(i * wide + j)

    turn_ks(0)
    pl.semaphore_wait(barrier, greeted)

    def send_k(i):
        pl.when(has_above)(lambda: up(0, 0, up_cuts[0][i]).start())

    send_k(0)
    loads[2].wait()
    for load in loads[3:]:
        load.start()
    stage[0 : rows * heads, :] = raw[0].astype(jnp.float32).reshape(rows * heads, width)
    turn_ks(1)
    for i in range(1, len(up_cuts[0])):
        if i + 1 < len(up_cuts[0]):
            turn_ks(i + 1)
        send_k(i)

    @pl.when(first)
    def _():
        for i in range(2):
            pass_across(0, 0, 0, i)

    loads[5].wait()
    row_at = me * rows + lax.broadcasted_iota(jnp.int32, (rows, rows), 0)
    start = jnp.zeros((rows, rows), jnp.int32)
    end = jnp.int32(0)
    for i in range(lengths.shape[1]):
        end = end + lengths[0, i]
        start = jnp.where(end <= row_at, end, start)
    low = jnp.maximum(start, row_at - (WINDOW - 1)) - me * rows
    query_at = lax.broadcasted_iota(jnp.int32, (rows, rows), 0)
    for d in range(reach + 1):
        key_at = lax.broadcasted_iota(jnp.int32, (rows, rows), 1) - d * rows
        bias[d] = jnp.where((key_at >= low) & (key_at <= query_at), 0.0, masked)

    loaded(load_sem.at[2], 2 * rows * heads * width, 2 * rows * q_heads * width)
    stage[...] = q_raw[...].astype(jnp.float32).reshape(rows * q_heads, width)
    scale = score_scale * math.log2(math.e)

    def turn_q(h):
        for g in range(group):
            x = stage[pl.ds(h * group + g, rows, stride=q_heads), :]
            turned = x * turn[0] + pltpu.roll(x, width // 2, 1) * turn[1]
            q_rot[h, g * rows : (g + 1) * rows, :] = (turned * scale).astype(jnp.bfloat16)

    each(0, heads, turn_q)

    stage[0 : rows * heads, :] = raw[1].astype(jnp.float32).reshape(rows * heads, width)

    def move_v(h):
        kv[1, 0, h] = stage[pl.ds(h, rows, stride=heads), :].astype(jnp.bfloat16)

    each(0, heads, move_v)

    @pl.when(first)
    def _():
        for i in range(2):
            pass_across(0, 1, 0, i)

    def score(d, h, fresh=False):
        s = lax.dot_general(
            q_rot[h], kv[0, d, h], (((1,), (1,)), ((), ())), preferred_element_type=jnp.float32
        )
        for g in range(group):
            part = slice(g * rows, (g + 1) * rows)
            t = s[part] + bias[d]
            scores[h, d, part, :] = t
            top = functools.reduce(jnp.maximum, [t[:, i * width : (i + 1) * width] for i in range(rows // width)])
            tops[h, part, :] = top if fresh else jnp.maximum(tops[h, part, :], top)

    def scores_of(d, i):
        each(i * half, (i + 1) * half, lambda h: score(d, h))

    each(0, heads, lambda h: score(0, h, fresh=True))

    @pl.when(second)
    def _():
        def step(i):
            take_across(0, 0, i)
            scores_of(1, i)

        for i in range(2):
            step(i)

    @pl.when(chip >= 1)
    def _():
        for i in range(2):
            take_up(0, 0, i)
            pl.when(has_above)(functools.partial(pass_up, 0, 1, i))
            pl.when(first)(functools.partial(pass_across, 0, 0, 1, i))
            pl.when(second)(functools.partial(pass_across, 1, 0, 1, i))
            scores_of(2, i)

    @pl.when(has_above)
    def _():
        for i in range(2):
            pass_up(1, 0, i)

    @pl.when(chip >= 1)
    def _():
        for i in range(2):
            pl.when(first)(functools.partial(take_across, 0, 0, i))
            pl.when(second)(functools.partial(take_across, 0, 1, i))
            scores_of(1 + 2 * core, i)

    @pl.when(chip >= 2)
    def _():
        for i in range(2):
            take_up(0, 1, i)
            pl.when(second)(functools.partial(pass_across, 1, 0, 2, i))
            scores_of(4, i)

        @pl.when(first)
        def _():
            for i in range(2):
                take_across(0, 1, i)
                scores_of(3, i)

    def finish(h, square, peak, total, part):
        shares[h, part, :] = jnp.broadcast_to(1.0 / total, (total.shape[0], width))
        lse = peak * math.log(2.0) + jnp.log(total)
        return square + jnp.sum(lse * lse, axis=0, keepdims=True)

    def weigh(h, square):
        for i in range(tall // TILE):
            part = slice(i * TILE, (i + 1) * TILE)
            peak = jnp.max(tops[h, part, :], axis=1, keepdims=True)
            total = jnp.zeros((TILE, width), jnp.float32)
            for d in range(reach + 1):
                p = jnp.exp2(scores[h, d, part, :] - peak)
                weights[h, d, part, :] = p.astype(jnp.bfloat16)
                for c in range(rows // width):
                    total = total + p[:, c * width : (c + 1) * width]
            square = finish(h, square, peak, jnp.sum(total, axis=1, keepdims=True), part)
        return square

    def weigh_some(h, square):
        for i in range(tall // TILE):
            part = slice(i * TILE, (i + 1) * TILE)
            peak = jnp.max(tops[h, part, :], axis=1, keepdims=True)

            def step(d, total):
                p = jnp.exp2(scores[h, d, part, :] - peak)
                weights[h, d, part, :] = p.astype(jnp.bfloat16)
                for c in range(rows // width):
                    total = total + p[:, c * width : (c + 1) * width]
                return total

            total = lax.fori_loop(0, blocks, step, jnp.zeros((TILE, width), jnp.float32))
            square = finish(h, square, peak, jnp.sum(total, axis=1, keepdims=True), part)
        return square

    def settle(square):
        mine[...] = jnp.broadcast_to(square, mine.shape)

    @pl.when(chip >= 2)
    def _():
        settle(lax.fori_loop(0, heads, weigh, jnp.zeros((1, 1), jnp.float32)))

    @pl.when(chip < 2)
    def _():
        settle(lax.fori_loop(0, heads, weigh_some, jnp.zeros((1, 1), jnp.float32)))

    def report(j):
        return remote(mine, parts_seq.at[j], s_sem.at[0], s_sem.at[1], "seq", 0)

    def tell_dp(j):
        return remote(mine2, parts_dp.at[dp], p_sem.at[0], p_sem.at[1], "dp", lax.rem(dp + j, n_dp))

    def tell(j):
        return remote(told, news, s_sem.at[0], s_sem.at[1], "seq", j)

    @pl.when(me > 0)
    def _():
        report(me).start()

    @pl.when(chip >= 1)
    def _():
        for i in range(2):
            take_up(1, 0, i)

            @pl.when(first)
            def _(i=i):
                pass_across(0, 1, 1, i)
                if i == 1:
                    for j in range(2):
                        take_across(1, 0, j)
                    pl.when(has_above)(lambda: lend_up().start())
                pl.when(has_above)(functools.partial(pass_up, 1, 1, i, short=i))

            @pl.when(second)
            def _(i=i):
                pl.when(has_above)(functools.partial(pass_up, 1, 1, i))
                pass_across(1, 1, 1, i)

    @pl.when(second)
    def _():
        for i in range(2):
            take_across(1, 0, i)

        @pl.when(chip >= 1)
        def _():
            for i in range(2):
                take_across(1, 1, i)

            @pl.when(has_above)
            def _():
                for j in range(2):
                    cross_up(j).start()

    def give(h, o):
        o = o * shares[h]
        for g in range(group):
            spread[pl.ds(h * group + g, rows, stride=q_heads), :] = o[g * rows : (g + 1) * rows]

    def blend(h, which):
        w = jnp.concatenate([weights[h, d] for d in which], axis=1)
        v = jnp.concatenate([kv[1, d, h] for d in which], axis=0)
        return jnp.dot(w, v, preferred_element_type=jnp.float32)

    def mix(h):
        give(h, tops[h] + blend(h, (reach - 1, reach)))

    def mix_early(h):
        tops[h] = blend(h, range(reach - 1))

    @pl.when(chip >= 2)
    def _():
        each(0, heads, mix_early)
        ups, acrosses = up_cuts[-1], across_cuts[-1]

        def mixed(cut):
            each(cut[1], cut[1] + cut[2], mix)

        @pl.when(first)
        def _():
            for j in range(2):
                up(1, 1, ups[j]).wait_recv()
                take_cut(1, 1, acrosses[j])
                mixed(ups[j])
                if j == 0:
                    lend_up().wait_recv()
                    lend_across().start()
                    tops[last] = tops[last] + blend(last, (reach - 1,))

            cross_up(0).wait_recv()
            take_cut(1, 1, acrosses[3])
            mixed(ups[3])
            up(1, 1, ups[2]).wait_recv()
            take_cut(1, 1, acrosses[2])
            mixed(ups[2])

        @pl.when(second)
        def _():
            tops[last] = tops[last] + blend(last, (reach - 1,))
            for j in range(4):
                up(1, 1, ups[j]).wait_recv()
                across(1, 1, 2, acrosses[j]).start()
                mixed(ups[j])

    @pl.when(chip < 2)
    def _():
        def mix_some(h):
            def step(d, o):
                return o + jnp.dot(weights[h, d], kv[1, d, h], preferred_element_type=jnp.float32)

            give(h, lax.fori_loop(0, blocks, step, jnp.zeros((tall, width), jnp.float32)))

        each(0, heads, mix_some)

    @pl.when(lead)
    def _():
        parts_seq[0] = mine[...]
        others, peers = parts_seq.at[pl.ds(1, n - 1)], parts_dp.at[pl.ds(1, n_dp - 1)]
        remote(others, others, s_sem.at[0], s_sem.at[1], "seq", other).wait_recv()
        column = jnp.sum(parts_seq[...], axis=0)
        mine2[...] = column
        parts_dp[dp] = column
        each(1, n_dp, lambda j: tell_dp(j).start())
        remote(peers, peers, p_sem.at[0], p_sem.at[1], "seq", other).wait_recv()
        whole = jnp.sum(parts_dp[...], axis=0) / (n_dp * n * rows * q_heads)
        told[...] = whole
        news[...] = whole
        each(1, n, lambda j: tell(j).start())
        remote(peers, peers, p_sem.at[0], p_sem.at[1], "seq", other).wait_send()
        remote(others, others, s_sem.at[0], s_sem.at[1], "seq", other).wait_send()

    @pl.when(me > 0)
    def _():
        tell(me).wait_recv()

    z_out[...] = news[...]

    def sent(view, sem):
        remote(view, view, sem, sem, "seq", other).wait_send()

    pl.when(has_above & (chip == 0))(lambda: sent(kv.at[0, 0:2], z_send.at[0]))
    pl.when(has_above & (chip >= 1))(lambda: sent(kv.at[0, 0:3], z_send.at[0]))
    pl.when(first & (chip == 0))(lambda: sent(kv.at[0, 0:2], d_send.at[0]))
    pl.when(first & (chip >= 1))(lambda: sent(kv.at[0, 0:4], d_send.at[0]))
    pl.when(second & (chip == 1))(lambda: sent(kv.at[0, 0:2], d_send.at[0]))
    pl.when(second & (chip >= 2))(lambda: sent(kv.at[0, 0:3], d_send.at[0]))

    @pl.when(me > 0)
    def _():
        report(me).wait_send()

    @pl.when(chip >= 2)
    def _():
        @pl.when(first)
        def _():
            cross_up(1).wait_recv()

        @pl.when(second)
        def _():
            lend_across().wait_recv()

        give(last, tops[last] + blend(last, (reach,)))

    pl.when(first & has_above & (chip >= 1))(lambda: sent(kv.at[1, 0, 0:last], z_send.at[1]))
    pl.when(second & has_above & (chip >= 1))(lambda: sent(kv.at[1, 0:3, 0 : (heads + 1) // 3], z_send.at[1]))
    pl.when(first & (chip >= 2))(lambda: sent(kv.at[1, 0, 0:1], d_send.at[1]))
    pl.when(second & (chip >= 2))(lambda: sent(kv.at[1, 0, 0:last], d_send.at[1]))


def place(held, z_held, out, z_out, rounded, z_one, sem):
    rows, q_heads, width = out.shape
    part = rows // PARTS
    for i in range(PARTS):
        at = slice(i * part, (i + 1) * part)
        x = held[i * part * q_heads : (i + 1) * part * q_heads, :]
        rounded[at] = x.reshape(part, q_heads, width).astype(jnp.bfloat16)
        pltpu.make_async_copy(rounded.at[at], out.at[at], sem.at[i]).start()
    z_one[...] = z_held[0:1, 0:1]
    z_copy = pltpu.make_async_copy(z_one, z_out, sem.at[PARTS])
    z_copy.start()
    for i in range(PARTS):
        at = slice(i * part, (i + 1) * part)
        pltpu.make_async_copy(rounded.at[at], out.at[at], sem.at[i]).wait()
    z_copy.wait()


def shards(queries, keys, values, lengths):
    _, rows, q_heads, width = queries.shape
    heads = keys.shape[2]
    group = q_heads // heads
    n = lax.axis_size("seq")
    n_dp = lax.axis_size("dp")
    reach = -(-(WINDOW - 1) // rows)
    assert n % 2 == 0 and reach == 4 and heads == 8
    hops = reach // 2
    tab = jnp.asarray(tables(rows, n, width))
    vmem = pl.BlockSpec(memory_space=pltpu.VMEM)
    anywhere = pl.BlockSpec(memory_space=pl.ANY)
    dma = pltpu.SemaphoreType.DMA
    out, z = pl.pallas_call(
        functools.partial(body, n, n_dp, reach),
        out_shape=(
            pltpu.VMEM((rows * q_heads, width), jnp.float32),
            pltpu.VMEM((8, width), jnp.float32),
        ),
        in_specs=[anywhere] * 5,
        out_specs=(vmem, vmem),
        scratch_shapes=[
            pltpu.SMEM(lengths.shape, jnp.int32),
            pltpu.VMEM(tab.shape, jnp.float32),
            pltpu.VMEM((2, rows, width), jnp.float32),
            pltpu.VMEM((rows, q_heads, width), jnp.bfloat16),
            pltpu.VMEM((rows, heads, width), jnp.bfloat16),
            pltpu.VMEM((2, rows, heads, width), jnp.bfloat16),
            pltpu.VMEM((rows * q_heads, width), jnp.float32),
            pltpu.VMEM((heads, group * rows, width), jnp.bfloat16),
            pltpu.VMEM((2, reach + 1, heads, rows, width), jnp.bfloat16),
            pltpu.VMEM((heads, reach + 1, group * rows, rows), jnp.float32),
            pltpu.VMEM((heads, reach + 1, group * rows, rows), jnp.bfloat16),
            pltpu.VMEM((heads, group * rows, width), jnp.float32),
            pltpu.VMEM((heads, group * rows, width), jnp.float32),
            pltpu.VMEM((reach + 1, rows, rows), jnp.float32),
            pltpu.VMEM((8, width), jnp.float32),
            pltpu.VMEM((n, 8, width), jnp.float32),
            pltpu.VMEM((8, width), jnp.float32),
            pltpu.VMEM((n_dp, 8, width), jnp.float32),
            pltpu.VMEM((8, width), jnp.float32),
            pltpu.VMEM((8, width), jnp.float32),
            dma((4,)),
            dma((2,)),
            dma((sum(len(cuts) for row in UP for cuts in row),)),
            dma((2,)),
            dma((sum(len(cuts) for row in ACROSS for cuts in row),)),
            dma((2,)),
            dma((2,)),
            dma((2,)),
        ],
        compiler_params=pltpu.CompilerParams(
            collective_id=0, has_side_effects=True, vmem_limit_bytes=56 * 1024 * 1024
        ),
        name="attend",
    )(lengths, queries[0], keys[0], values[0], tab)
    out, z = pl.pallas_call(
        place,
        out_shape=(
            jax.ShapeDtypeStruct((rows, q_heads, width), jnp.bfloat16),
            jax.ShapeDtypeStruct((1, 1), jnp.float32),
        ),
        in_specs=[vmem, vmem],
        out_specs=(anywhere, anywhere),
        scratch_shapes=[
            pltpu.VMEM((rows, q_heads, width), jnp.bfloat16), pltpu.VMEM((1, 1), jnp.float32), dma((PARTS + 1,))
        ],
        compiler_params=pltpu.CompilerParams(vmem_limit_bytes=4 * 1024 * 1024),
        name="place",
    )(out, z)
    return out[None], z[0, 0]


def solution(mesh):
    placed = (
        P("dp", "seq", None, None),
        P("dp", "seq", None, None),
        P("dp", "seq", None, None),
        P("dp", None),
    )
    return jax.shard_map(
        shards,
        mesh=mesh,
        in_specs=placed,
        out_specs=(P("dp", "seq", None, None), P()),
        check_vma=False,
    )
```

```python
import functools
import math

import jax
import jax.numpy as jnp
import numpy as np
from jax import lax
from jax.experimental import pallas as pl
from jax.experimental.pallas import tpu as pltpu
from jax.sharding import PartitionSpec as P

WINDOW = 1024
rope_base = 500000.0
score_scale = 1.0 / 12.0
masked = -1e30
MESH = pl.DeviceIdType.MESH
TILE = 64
PARTS = 4
UP = (((2, 2, 2, 2), (4, 4)), ((4, 4), (4, 1, 1, 1)))
ACROSS = (((4, 4), (4, 4)), ((4, 4), (4, 1, 1, 1, 1)))


def tables(rows, n, width):
    half = width // 2
    frequency = rope_base ** (-2.0 * np.arange(half) / width)
    at = np.concatenate([np.arange(rows), rows * np.arange(-(-n // 8) * 8)])
    angles = at[:, None] * frequency
    cos = np.concatenate([np.cos(angles)] * 2, axis=-1)
    sin = np.concatenate([-np.sin(angles), np.sin(angles)], axis=-1)
    return np.stack([cos, sin]).astype(np.float32)


def body(
    n, n_dp, reach, lengths_hbm, q_hbm, k_hbm, v_hbm, tab_hbm, spread, z_out,
    lengths, tab, turn, q_raw, lead_raw, raw, stage, q_rot, kv, scores, weights, tops, shares, bias,
    mine, parts_seq, mine2, parts_dp, told, news,
    load_sem, z_send, z_recv, d_send, d_recv, x_recv, s_sem, p_sem,
):
    rows, heads, width = k_hbm.shape
    q_heads = q_hbm.shape[1]
    group = q_heads // heads
    tall = group * rows
    hops = reach // 2
    me = lax.axis_index("seq")
    dp = lax.axis_index("dp")
    core = lax.rem(me, 2)
    chip = me // 2
    other = me + 1 - 2 * core
    above = me + 2
    has_above = above < n
    first = core == 0
    second = core == 1
    blocks = jnp.minimum(me, reach) + 1

    wide = heads // len(UP[0][0])
    loads = [
        pltpu.make_async_copy(k_hbm.at[:, 0:wide], lead_raw.at[:, 0:wide], load_sem.at[0]),
        pltpu.make_async_copy(tab_hbm, tab, load_sem.at[0]),
        pltpu.make_async_copy(k_hbm, raw.at[0], load_sem.at[1]),
        pltpu.make_async_copy(v_hbm, raw.at[1], load_sem.at[2]),
        pltpu.make_async_copy(q_hbm, q_raw, load_sem.at[2]),
        pltpu.make_async_copy(lengths_hbm, lengths, load_sem.at[3]),
    ]
    barrier = pltpu.get_barrier_semaphore()

    def greet(axis, at):
        pl.semaphore_signal(barrier, inc=1, device_id={axis: at}, device_id_type=MESH)

    def each(low_i, high_i, do):
        def step(i, _):
            do(i)
            return 0

        lax.fori_loop(low_i, high_i, step, 0)

    has_below = me >= 2
    far = me >= 3
    lead = me == 0
    pl.when(has_below)(lambda: greet("seq", me - 2))
    for load in loads[:3]:
        load.start()

    greet("seq", other)
    pl.when(has_above)(lambda: greet("seq", above))

    @pl.when(lead)
    def _():
        each(3, n, lambda j: greet("seq", j))
        each(1, n_dp, lambda j: greet("dp", lax.rem(dp + j, n_dp)))

    greeted = 1 + has_above.astype(jnp.int32) + has_below.astype(jnp.int32) + far.astype(jnp.int32)
    greeted = greeted + lead.astype(jnp.int32) * (n_dp - 1)

    def lay(table):
        count = 0
        laid = []
        for row in table:
            for eighths in row:
                at, cuts = 0, []
                for size in eighths:
                    cuts.append((count, at * heads // 8, size * heads // 8))
                    count, at = count + 1, at + size
                laid.append(cuts)
        return laid

    up_cuts, across_cuts = lay(UP), lay(ACROSS)

    def remote(src, dst, send, recv, axis, at):
        return pltpu.make_async_remote_copy(
            src_ref=src, dst_ref=dst, send_sem=send, recv_sem=recv, device_id={axis: at}, device_id_type=MESH
        )

    def some(kind, d, i, size):
        return kv.at[kind, d, pl.ds(i, size)]

    def up(kind, hop, cut):
        at, start, size = cut
        late = kind * hop
        return remote(
            some(kind, 2 * hop, start, size), some(kind, 2 * hop + 2, start, size),
            z_send.at[late], z_recv.at[at], "seq", above,
        )

    def across(side, kind, hop, cut):
        at, start, size = cut
        late = int(kind == 1 and hop == 2)
        return remote(
            some(kind, 2 * hop, start, size), some(kind, 2 * hop + 1 - 2 * side, start, size),
            d_send.at[late], d_recv.at[at], "seq", other,
        )

    last = heads - 1

    def lend_up():
        return remote(some(1, 1, last, 1), some(1, 3, last, 1), z_send.at[1], x_recv.at[0], "seq", above)

    def lend_across():
        return remote(some(1, 3, last, 1), some(1, 4, last, 1), d_send.at[1], x_recv.at[0], "seq", other)

    def cross_up(j):
        h = last - 1 + j
        landed = x_recv.at[1] if j else z_recv.at[up_cuts[-1][-1][0]]
        return remote(some(1, 3, h, 1), some(1, 4, h, 1), z_send.at[1], landed, "seq", me + 1)

    half = heads // 2

    def cuts_of(cuts, i):
        return [cut for cut in cuts if i * half <= cut[1] < (i + 1) * half]

    def take_up(kind, hop, i):
        for cut in cuts_of(up_cuts[kind * hops + hop], i):
            up(kind, hop, cut).wait_recv()

    def take_cut(kind, slot, cut):
        at, start, size = cut
        remote(
            some(kind, 0, start, size), some(kind, 2 * slot + 1, start, size),
            d_send.at[0], d_recv.at[at], "seq", other,
        ).wait_recv()

    def take_across(kind, slot, i):
        for cut in cuts_of(across_cuts[kind * hops + slot], i):
            take_cut(kind, slot, cut)

    def pass_across(side, kind, hop, i):
        for cut in cuts_of(across_cuts[kind * hops + hop - side], i):
            across(side, kind, hop, cut).start()

    def pass_up(kind, hop, i, short=0):
        cuts = cuts_of(up_cuts[kind * hops + hop], i)
        for cut in cuts[: len(cuts) - short]:
            up(kind, hop, cut).start()

    def loaded(sem, *sizes):
        view = stage.at[0 : sum(sizes) // (4 * width)]
        pltpu.make_async_copy(view, view, sem).wait()

    loaded(load_sem.at[0], 2 * rows * wide * width, 4 * 2 * tab.shape[1] * width)
    cos_b = tab[0, pl.ds(rows + me, 1), :]
    sin_b = tab[1, pl.ds(rows + me, 1), :]
    turn[0] = tab[0, 0:rows, :] * cos_b - tab[1, 0:rows, :] * sin_b
    turn[1] = tab[1, 0:rows, :] * cos_b + tab[0, 0:rows, :] * sin_b
    stage[0 : rows * heads, :] = lead_raw[...].astype(jnp.float32).reshape(rows * heads, width)

    def turn_k(h):
        x = stage[pl.ds(h, rows, stride=heads), :]
        kv[0, 0, h] = (x * turn[0] + pltpu.roll(x, width // 2, 1) * turn[1]).astype(jnp.bfloat16)

    def turn_ks(i):
        for j in range(wide):
            turn_k(i * wide + j)

    turn_ks(0)
    pl.semaphore_wait(barrier, greeted)

    def send_k(i):
        pl.when(has_above)(lambda: up(0, 0, up_cuts[0][i]).start())

    send_k(0)
    loads[2].wait()
    for load in loads[3:]:
        load.start()
    stage[0 : rows * heads, :] = raw[0].astype(jnp.float32).reshape(rows * heads, width)
    turn_ks(1)
    for i in range(1, len(up_cuts[0])):
        if i + 1 < len(up_cuts[0]):
            turn_ks(i + 1)
        send_k(i)

    @pl.when(first)
    def _():
        for i in range(2):
            pass_across(0, 0, 0, i)

    loads[5].wait()
    row_at = me * rows + lax.broadcasted_iota(jnp.int32, (rows, rows), 0)
    start = jnp.zeros((rows, rows), jnp.int32)
    end = jnp.int32(0)
    for i in range(lengths.shape[1]):
        end = end + lengths[0, i]
        start = jnp.where(end <= row_at, end, start)
    low = jnp.maximum(start, row_at - (WINDOW - 1)) - me * rows
    query_at = lax.broadcasted_iota(jnp.int32, (rows, rows), 0)
    for d in range(reach + 1):
        key_at = lax.broadcasted_iota(jnp.int32, (rows, rows), 1) - d * rows
        bias[d] = jnp.where((key_at >= low) & (key_at <= query_at), 0.0, masked)

    loaded(load_sem.at[2], 2 * rows * heads * width, 2 * rows * q_heads * width)
    stage[...] = q_raw[...].astype(jnp.float32).reshape(rows * q_heads, width)
    scale = score_scale * math.log2(math.e)

    def turn_q(h):
        for g in range(group):
            x = stage[pl.ds(h * group + g, rows, stride=q_heads), :]
            turned = x * turn[0] + pltpu.roll(x, width // 2, 1) * turn[1]
            q_rot[h, g * rows : (g + 1) * rows, :] = (turned * scale).astype(jnp.bfloat16)

    each(0, heads, turn_q)

    stage[0 : rows * heads, :] = raw[1].astype(jnp.float32).reshape(rows * heads, width)

    def move_v(h):
        kv[1, 0, h] = stage[pl.ds(h, rows, stride=heads), :].astype(jnp.bfloat16)

    each(0, heads, move_v)

    @pl.when(first)
    def _():
        for i in range(2):
            pass_across(0, 1, 0, i)

    def score(d, h, fresh=False):
        s = lax.dot_general(
            q_rot[h], kv[0, d, h], (((1,), (1,)), ((), ())), preferred_element_type=jnp.float32
        )
        for g in range(group):
            part = slice(g * rows, (g + 1) * rows)
            t = s[part] + bias[d]
            scores[h, d, part, :] = t
            top = functools.reduce(jnp.maximum, [t[:, i * width : (i + 1) * width] for i in range(rows // width)])
            tops[h, part, :] = top if fresh else jnp.maximum(tops[h, part, :], top)

    def scores_of(d, i):
        each(i * half, (i + 1) * half, lambda h: score(d, h))

    each(0, heads, lambda h: score(0, h, fresh=True))

    @pl.when(second)
    def _():
        def step(i):
            take_across(0, 0, i)
            scores_of(1, i)

        for i in range(2):
            step(i)

    @pl.when(chip >= 1)
    def _():
        for i in range(2):
            take_up(0, 0, i)
            pl.when(has_above)(functools.partial(pass_up, 0, 1, i))
            pl.when(first)(functools.partial(pass_across, 0, 0, 1, i))
            pl.when(second)(functools.partial(pass_across, 1, 0, 1, i))
            scores_of(2, i)

    @pl.when(has_above)
    def _():
        for i in range(2):
            pass_up(1, 0, i)

    @pl.when(chip >= 1)
    def _():
        for i in range(2):
            pl.when(first)(functools.partial(take_across, 0, 0, i))
            pl.when(second)(functools.partial(take_across, 0, 1, i))
            scores_of(1 + 2 * core, i)

    @pl.when(chip >= 2)
    def _():
        for i in range(2):
            take_up(0, 1, i)
            pl.when(second)(functools.partial(pass_across, 1, 0, 2, i))
            scores_of(4, i)

        @pl.when(first)
        def _():
            for i in range(2):
                take_across(0, 1, i)
                scores_of(3, i)

    def finish(h, square, peak, total, part):
        shares[h, part, :] = jnp.broadcast_to(1.0 / total, (total.shape[0], width))
        lse = peak * math.log(2.0) + jnp.log(total)
        return square + jnp.sum(lse * lse, axis=0, keepdims=True)

    def weigh(h, square):
        for i in range(tall // TILE):
            part = slice(i * TILE, (i + 1) * TILE)
            peak = jnp.max(tops[h, part, :], axis=1, keepdims=True)
            total = jnp.zeros((TILE, width), jnp.float32)
            for d in range(reach + 1):
                p = jnp.exp2(scores[h, d, part, :] - peak)
                weights[h, d, part, :] = p.astype(jnp.bfloat16)
                for c in range(rows // width):
                    total = total + p[:, c * width : (c + 1) * width]
            square = finish(h, square, peak, jnp.sum(total, axis=1, keepdims=True), part)
        return square

    def weigh_some(h, square):
        for i in range(tall // TILE):
            part = slice(i * TILE, (i + 1) * TILE)
            peak = jnp.max(tops[h, part, :], axis=1, keepdims=True)

            def step(d, total):
                p = jnp.exp2(scores[h, d, part, :] - peak)
                weights[h, d, part, :] = p.astype(jnp.bfloat16)
                for c in range(rows // width):
                    total = total + p[:, c * width : (c + 1) * width]
                return total

            total = lax.fori_loop(0, blocks, step, jnp.zeros((TILE, width), jnp.float32))
            square = finish(h, square, peak, jnp.sum(total, axis=1, keepdims=True), part)
        return square

    def settle(square):
        mine[...] = jnp.broadcast_to(square, mine.shape)

    @pl.when(chip >= 2)
    def _():
        settle(lax.fori_loop(0, heads, weigh, jnp.zeros((1, 1), jnp.float32)))

    @pl.when(chip < 2)
    def _():
        settle(lax.fori_loop(0, heads, weigh_some, jnp.zeros((1, 1), jnp.float32)))

    def report(j):
        return remote(mine, parts_seq.at[j], s_sem.at[0], s_sem.at[1], "seq", 0)

    def tell_dp(j):
        return remote(mine2, parts_dp.at[dp], p_sem.at[0], p_sem.at[1], "dp", lax.rem(dp + j, n_dp))

    def tell(j):
        return remote(told, news, s_sem.at[0], s_sem.at[1], "seq", j)

    @pl.when(me > 0)
    def _():
        report(me).start()

    @pl.when(chip >= 1)
    def _():
        for i in range(2):
            take_up(1, 0, i)

            @pl.when(first)
            def _(i=i):
                pass_across(0, 1, 1, i)
                if i == 1:
                    for j in range(2):
                        take_across(1, 0, j)
                    pl.when(has_above)(lambda: lend_up().start())
                pl.when(has_above)(functools.partial(pass_up, 1, 1, i, short=i))

            @pl.when(second)
            def _(i=i):
                pl.when(has_above)(functools.partial(pass_up, 1, 1, i))
                pass_across(1, 1, 1, i)

    @pl.when(second)
    def _():
        for i in range(2):
            take_across(1, 0, i)

        @pl.when(chip >= 1)
        def _():
            for i in range(2):
                take_across(1, 1, i)

            @pl.when(has_above)
            def _():
                for j in range(2):
                    cross_up(j).start()

    def give(h, o):
        o = o * shares[h]
        for g in range(group):
            spread[pl.ds(h * group + g, rows, stride=q_heads), :] = o[g * rows : (g + 1) * rows]

    def blend(h, which):
        w = jnp.concatenate([weights[h, d] for d in which], axis=1)
        v = jnp.concatenate([kv[1, d, h] for d in which], axis=0)
        return jnp.dot(w, v, preferred_element_type=jnp.float32)

    def mix(h):
        give(h, tops[h] + blend(h, (reach - 1, reach)))

    def mix_early(h):
        tops[h] = blend(h, range(reach - 1))

    @pl.when(chip >= 2)
    def _():
        each(0, heads, mix_early)
        ups, acrosses = up_cuts[-1], across_cuts[-1]

        def mixed(cut):
            each(cut[1], cut[1] + cut[2], mix)

        @pl.when(first)
        def _():
            for j in range(2):
                up(1, 1, ups[j]).wait_recv()
                take_cut(1, 1, acrosses[j])
                mixed(ups[j])
                if j == 0:
                    lend_up().wait_recv()
                    lend_across().start()
                    tops[last] = tops[last] + blend(last, (reach - 1,))

            cross_up(0).wait_recv()
            take_cut(1, 1, acrosses[3])
            mixed(ups[3])
            up(1, 1, ups[2]).wait_recv()
            take_cut(1, 1, acrosses[2])
            mixed(ups[2])

        @pl.when(second)
        def _():
            tops[last] = tops[last] + blend(last, (reach - 1,))
            for j in range(4):
                up(1, 1, ups[j]).wait_recv()
                across(1, 1, 2, acrosses[j]).start()
                mixed(ups[j])

    @pl.when(chip < 2)
    def _():
        def mix_some(h):
            def step(d, o):
                return o + jnp.dot(weights[h, d], kv[1, d, h], preferred_element_type=jnp.float32)

            give(h, lax.fori_loop(0, blocks, step, jnp.zeros((tall, width), jnp.float32)))

        each(0, heads, mix_some)

    @pl.when(lead)
    def _():
        parts_seq[0] = mine[...]
        others, peers = parts_seq.at[pl.ds(1, n - 1)], parts_dp.at[pl.ds(1, n_dp - 1)]
        remote(others, others, s_sem.at[0], s_sem.at[1], "seq", other).wait_recv()
        column = jnp.sum(parts_seq[...], axis=0)
        mine2[...] = column
        parts_dp[dp] = column
        each(1, n_dp, lambda j: tell_dp(j).start())
        remote(peers, peers, p_sem.at[0], p_sem.at[1], "seq", other).wait_recv()
        whole = jnp.sum(parts_dp[...], axis=0) / (n_dp * n * rows * q_heads)
        told[...] = whole
        news[...] = whole
        each(1, n, lambda j: tell(j).start())
        remote(peers, peers, p_sem.at[0], p_sem.at[1], "seq", other).wait_send()
        remote(others, others, s_sem.at[0], s_sem.at[1], "seq", other).wait_send()

    @pl.when(me > 0)
    def _():
        tell(me).wait_recv()

    z_out[...] = news[...]

    def sent(view, sem):
        remote(view, view, sem, sem, "seq", other).wait_send()

    pl.when(has_above & (chip == 0))(lambda: sent(kv.at[0, 0:2], z_send.at[0]))
    pl.when(has_above & (chip >= 1))(lambda: sent(kv.at[0, 0:3], z_send.at[0]))
    pl.when(first & (chip == 0))(lambda: sent(kv.at[0, 0:2], d_send.at[0]))
    pl.when(first & (chip >= 1))(lambda: sent(kv.at[0, 0:4], d_send.at[0]))
    pl.when(second & (chip == 1))(lambda: sent(kv.at[0, 0:2], d_send.at[0]))
    pl.when(second & (chip >= 2))(lambda: sent(kv.at[0, 0:3], d_send.at[0]))

    @pl.when(me > 0)
    def _():
        report(me).wait_send()

    @pl.when(chip >= 2)
    def _():
        @pl.when(first)
        def _():
            cross_up(1).wait_recv()

        @pl.when(second)
        def _():
            lend_across().wait_recv()

        give(last, tops[last] + blend(last, (reach,)))

    pl.when(first & has_above & (chip >= 1))(lambda: sent(kv.at[1, 0, 0:last], z_send.at[1]))
    pl.when(second & has_above & (chip >= 1))(lambda: sent(kv.at[1, 0:3, 0 : (heads + 1) // 3], z_send.at[1]))
    pl.when(first & (chip >= 2))(lambda: sent(kv.at[1, 0, 0:1], d_send.at[1]))
    pl.when(second & (chip >= 2))(lambda: sent(kv.at[1, 0, 0:last], d_send.at[1]))


def place(held, z_held, out, z_out, rounded, z_one, sem):
    rows, q_heads, width = out.shape
    part = rows // PARTS
    for i in range(PARTS):
        at = slice(i * part, (i + 1) * part)
        x = held[i * part * q_heads : (i + 1) * part * q_heads, :]
        rounded[at] = x.reshape(part, q_heads, width).astype(jnp.bfloat16)
        pltpu.make_async_copy(rounded.at[at], out.at[at], sem.at[i]).start()
    z_one[...] = z_held[0:1, 0:1]
    z_copy = pltpu.make_async_copy(z_one, z_out, sem.at[PARTS])
    z_copy.start()
    for i in range(PARTS):
        at = slice(i * part, (i + 1) * part)
        pltpu.make_async_copy(rounded.at[at], out.at[at], sem.at[i]).wait()
    z_copy.wait()


def shards(queries, keys, values, lengths):
    _, rows, q_heads, width = queries.shape
    heads = keys.shape[2]
    group = q_heads // heads
    n = lax.axis_size("seq")
    n_dp = lax.axis_size("dp")
    reach = -(-(WINDOW - 1) // rows)
    assert n % 2 == 0 and reach == 4 and heads == 8
    hops = reach // 2
    tab = jnp.asarray(tables(rows, n, width))
    vmem = pl.BlockSpec(memory_space=pltpu.VMEM)
    anywhere = pl.BlockSpec(memory_space=pl.ANY)
    dma = pltpu.SemaphoreType.DMA
    out, z = pl.pallas_call(
        functools.partial(body, n, n_dp, reach),
        out_shape=(
            pltpu.VMEM((rows * q_heads, width), jnp.float32),
            pltpu.VMEM((8, width), jnp.float32),
        ),
        in_specs=[anywhere] * 5,
        out_specs=(vmem, vmem),
        scratch_shapes=[
            pltpu.SMEM(lengths.shape, jnp.int32),
            pltpu.VMEM(tab.shape, jnp.float32),
            pltpu.VMEM((2, rows, width), jnp.float32),
            pltpu.VMEM((rows, q_heads, width), jnp.bfloat16),
            pltpu.VMEM((rows, heads, width), jnp.bfloat16),
            pltpu.VMEM((2, rows, heads, width), jnp.bfloat16),
            pltpu.VMEM((rows * q_heads, width), jnp.float32),
            pltpu.VMEM((heads, group * rows, width), jnp.bfloat16),
            pltpu.VMEM((2, reach + 1, heads, rows, width), jnp.bfloat16),
            pltpu.VMEM((heads, reach + 1, group * rows, rows), jnp.float32),
            pltpu.VMEM((heads, reach + 1, group * rows, rows), jnp.bfloat16),
            pltpu.VMEM((heads, group * rows, width), jnp.float32),
            pltpu.VMEM((heads, group * rows, width), jnp.float32),
            pltpu.VMEM((reach + 1, rows, rows), jnp.float32),
            pltpu.VMEM((8, width), jnp.float32),
            pltpu.VMEM((n, 8, width), jnp.float32),
            pltpu.VMEM((8, width), jnp.float32),
            pltpu.VMEM((n_dp, 8, width), jnp.float32),
            pltpu.VMEM((8, width), jnp.float32),
            pltpu.VMEM((8, width), jnp.float32),
            dma((4,)),
            dma((2,)),
            dma((sum(len(cuts) for row in UP for cuts in row),)),
            dma((2,)),
            dma((sum(len(cuts) for row in ACROSS for cuts in row),)),
            dma((2,)),
            dma((2,)),
            dma((2,)),
        ],
        compiler_params=pltpu.CompilerParams(
            collective_id=0, has_side_effects=True, vmem_limit_bytes=56 * 1024 * 1024,
        ),
        name="attend",
    )(lengths, queries[0], keys[0], values[0], tab)
    out, z = pl.pallas_call(
        place,
        out_shape=(
            jax.ShapeDtypeStruct((rows, q_heads, width), jnp.bfloat16),
            jax.ShapeDtypeStruct((1, 1), jnp.float32),
        ),
        in_specs=[vmem, vmem],
        out_specs=(anywhere, anywhere),
        scratch_shapes=[
            pltpu.VMEM((rows, q_heads, width), jnp.bfloat16), pltpu.VMEM((1, 1), jnp.float32), dma((PARTS + 1,))
        ],
        compiler_params=pltpu.CompilerParams(vmem_limit_bytes=4 * 1024 * 1024),
        name="place",
    )(out, z)
    return out[None], z[0, 0]


def solution(mesh):
    placed = (
        P("dp", "seq", None, None),
        P("dp", "seq", None, None),
        P("dp", "seq", None, None),
        P("dp", None),
    )
    return jax.shard_map(
        shards,
        mesh=mesh,
        in_specs=placed,
        out_specs=(P("dp", "seq", None, None), P()),
        check_vma=False,
    )
```
